32 devices in a mesh: blk: 32 (over z, y, x, core).
Axes of the slice: x: 2, y: 2, z: 4, core: 2. Of those that a mesh axis runs over, the one named last changes fastest.
Arguments:
- defect: float32 [384, 128], P('blk'), may hold values from -6 to 6
- mass: float32 [384, 128], P('blk'), may hold values from 1 to 2
- block_diag: float32 [384, 128, 128], P('blk'), may hold values from -0.1875 to 0.1875
- coupling: float32 [3072, 128, 128], P('blk'), may hold values from -0.09375 to 0.09375
- tile_rows: int32 [3072], P('blk'), may hold values from 0 to 383, as said below
- tile_cols: int32 [3072], P('blk'), may hold values from 0 to 383, as said below
Outputs:
- update: float32 [384, 128], P('blk')
The draws below stay inside these ranges and needn't reach their ends.
Inputs may be any that keep to these rules, and one draw needn't show every extreme that they name: `tile_rows`: block rows d * 12 to d * 12 + 11 belong to device d of blk, and each device holds the tiles at positions d * 96 to d * 96 + 95. Of every tile a device holds, exactly one of its block row and block column belongs to that device; the other belongs to a different device. Exactly half of the 96 tiles of every device have their block row with that device, and the other half their block column. A program may send only the blocks and products of tiles that exist; slots of a padded buffer that no tile fills need not be sent. `tile_cols`: of one device's tiles, at most 2 have their block column with any one other device and at most 2 have their block row with any one other device; every device reaches 2 with some other device on each of the two sides.
All inputs are finite; a program needn't handle non-finite values.
Results may differ from the reference program's by a relative error of at most 0.0001.
Values sent between devices are 32-bit elements; how exact they have to be, the bound alone decides.
A program may use at most 64 MiB of HBM per device.

```python
import jax
import jax.numpy as jnp
from jax import lax

B = 128
K = 8
RB = 12
ITERS = 3
TD = 96
C = 2
NB = 384
NT = 3072
N_BLK = 32


def tile_pattern(key):
    base = jax.random.fold_in(key, 11)
    half = TD // 2
    peers = N_BLK - 1
    cells = peers * C
    antipode_lane = N_BLK // 2 - 1

    def one_device(device_key, device):
        keys = jax.random.split(device_key, 6)

        def pick(pick_key):
            order = jax.random.permutation(pick_key, cells).astype(jnp.int32)
            grid = jnp.arange(cells, dtype=jnp.int32)
            score = jnp.where(grid // C == antipode_lane, grid - cells, order)
            return (jnp.argsort(score, stable=True)[:half] // C).astype(jnp.int32)
        lanes = jnp.concatenate([pick(keys[1]), pick(keys[2])])
        far_device = (device + lanes + 1) % N_BLK
        own_slot = jax.random.randint(keys[3], (TD,), 0, RB).astype(jnp.int32)
        far_slot = jax.random.randint(keys[4], (TD,), 0, RB).astype(jnp.int32)
        own_block = device * RB + own_slot
        far_block = far_device * RB + far_slot
        first = jnp.arange(TD) < half
        rows = jnp.where(first, own_block, far_block)
        cols = jnp.where(first, far_block, own_block)
        shuffle = jax.random.permutation(keys[5], TD)
        return (rows[shuffle], cols[shuffle])
    owners = jnp.arange(N_BLK, dtype=jnp.int32)
    rows, cols = jax.vmap(one_device)(jax.random.split(base, N_BLK), owners)
    return (rows.reshape(NT).astype(jnp.int32), cols.reshape(NT).astype(jnp.int32))


def draw_tile_rows(key, part):
    return tile_pattern(key)[0]


def draw_tile_cols(key, part):
    return tile_pattern(key)[1]


def levels(rng, dims, cuts, least, top_value):
    def one(axis_at, blocks):
        steps = jax.random.uniform(jax.random.fold_in(jax.random.fold_in(rng, 6), axis_at), (blocks,), jnp.float32, least / len(cuts), top_value / len(cuts))
        return jnp.repeat(jnp.exp(steps), dims[axis_at] // blocks).reshape((-1,) + (1,) * (len(dims) - axis_at - 1))

    loudness = one(*cuts[0])
    for cut in cuts[1:]:
        loudness = loudness * one(*cut)
    return loudness


def gaussian(key, shape, scale, limit, cuts=(), held_as=jnp.bfloat16):
    drawn = jax.random.normal(key, shape, jnp.float32) * scale
    if len(cuts) > 0:
        drawn = levels(key, shape, cuts, -0.22, 0.18) * drawn
    return jnp.clip(drawn, min=-limit, max=limit).astype(held_as)


def setup_inputs(seed: int = 0) -> dict:
    splits = jax.random.split(jax.random.key(seed), 7)
    return {
        "defect": gaussian(splits[0], (NB, B), 1.0, 6.0, ((0, 32),), jnp.float32),
        "mass": jnp.clip(1.0 + 1.0 * jax.random.uniform(splits[1], (NB, B), jnp.float32) ** levels(splits[1], (NB, B), ((0, 32),), -0.2, 0.2), 1.0, 2.0),
        "block_diag": gaussian(splits[2], (NB, B, B), (8 * B) ** -0.5, 0.1875, ((0, 32),), jnp.float32),
        "coupling": gaussian(splits[3], (NT, B, B), (4 * K * B) ** -0.5, 0.09375, ((0, 32),), jnp.float32),
        "tile_rows": draw_tile_rows(jax.random.fold_in(splits[6], 71), 0),
        "tile_cols": draw_tile_cols(jax.random.fold_in(splits[6], 71), 0),
    }


def solve_small(gram, target):
    factor = jnp.linalg.cholesky(gram)
    count = gram.shape[0]
    forward = []
    for index in range(count):
        value = target[index]
        for inner in range(index):
            value = value - factor[index, inner] * forward[inner]
        forward.append(value / factor[index, index])
    backward = [None] * count
    for index in reversed(range(count)):
        value = forward[index]
        for inner in range(index + 1, count):
            value = value - factor[inner, index] * backward[inner]
        backward[index] = value / factor[index, index]
    return backward

def newton_apply(vector, mass, block_diag, coupling, tile_rows, tile_cols):
    own = jnp.einsum('rij,rj->ri', block_diag, vector, precision=lax.Precision.HIGHEST)
    products = jnp.einsum('tij,tj->ti', coupling, vector[tile_cols], precision=lax.Precision.HIGHEST)
    far = jax.ops.segment_sum(products, tile_rows, num_segments=NB)
    return mass * vector + own + far

def reference(defect, mass, block_diag, coupling, tile_rows, tile_cols):
    negated = -defect
    beta = jnp.sqrt(jnp.sum(negated * negated))
    basis = [negated / beta]
    upper = jnp.zeros((ITERS + 1, ITERS), jnp.float32)
    for column in range(ITERS):
        image = newton_apply(basis[column], mass, block_diag, coupling, tile_rows, tile_cols)
        dots = jnp.stack([jnp.sum(item * image) for item in basis])
        for index in range(column + 1):
            image = image - dots[index] * basis[index]
        norm = jnp.sqrt(jnp.sum(image * image))
        upper = upper.at[:column + 1, column].set(dots)
        upper = upper.at[column + 1, column].set(norm)
        if column + 1 < ITERS:
            basis.append(image / norm)
    gram = jnp.dot(upper.T.astype(jnp.float32), upper.astype(jnp.float32), precision=lax.Precision.HIGHEST, preferred_element_type=jnp.float32)
    mixing = solve_small(gram, beta * upper[0, :])
    update = jnp.zeros_like(defect)
    for index in range(ITERS):
        update = update + mixing[index] * basis[index]
    return update
```

```python
import functools

import jax
import jax.numpy as jnp
from jax import lax
from jax.experimental import pallas as pl
from jax.experimental.pallas import tpu as pltpu
from jax.sharding import PartitionSpec as P

ITERS = 3
F32 = jnp.float32
I32 = jnp.int32
MESH = pl.DeviceIdType.MESH
BASE = 64
VMEM_LIMIT = 48 * 1024 * 1024


def iota(shape, axis):
    return lax.broadcasted_iota(I32, shape, axis)


def iota_f(shape, axis):
    return iota(shape, axis).astype(F32)


def total(value):
    return jnp.sum(jnp.sum(value, axis=0, keepdims=True), axis=1, keepdims=True)


def as_row(items):
    lane = iota((1, 128), 1)
    row = jnp.zeros((1, 128), F32)
    for index, item in enumerate(items):
        row = jnp.where(lane == index, item, row)
    return row


def pick(row, index):
    lane = iota((1, 128), 1)
    return jnp.sum(jnp.where(lane == index, row, 0.0), axis=1, keepdims=True)


def ranges(n):
    cuts = [0, 2, 6, 10, n // 2, n - n // 4, n - 1]
    cuts = sorted({min(cut, n - 1) for cut in cuts})
    return list(zip(cuts[:-1], cuts[1:]))


def kernel(
    n,
    slots,
    defect_hbm,
    mass_hbm,
    diag_hbm,
    coup_hbm,
    rows_hbm,
    cols_hbm,
    out_ref,
    coup,
    diag,
    defect_ref,
    mass_ref,
    rows_ref,
    cols_ref,
    table_v,
    table,
    wbuf,
    codes,
    ask_ref,
    goal_ref,
    send0,
    recv0,
    blocks,
    send_a,
    recv_a,
    send_b,
    recv_b,
    send_f,
    recv_f,
    load_sems,
    table_sem,
    sent,
    got,
):
    me = lax.axis_index("blk")
    rb, width = defect_ref.shape
    tiles = rows_ref.shape[1]
    pad = wbuf.shape[0]
    lanes = table.shape[1]
    parts = 4
    chunk = tiles // parts
    groups = ranges(n)
    count = len(groups)
    head = rb + 1
    lines = slots + 1

    peers = {0: me}
    for mask in range(1, n):
        low_bit = mask & -mask
        sign = 1 - 2 * ((me // low_bit) % 2)
        peers[mask] = peers[mask - low_bit] + sign * low_bit
    peer = [peers[n - 1 - place] for place in range(n)]

    small = [
        pltpu.make_async_copy(rows_hbm, rows_ref, load_sems.at[parts + 1]),
        pltpu.make_async_copy(cols_hbm, cols_ref, load_sems.at[parts + 2]),
        pltpu.make_async_copy(defect_hbm, defect_ref, load_sems.at[parts + 3]),
        pltpu.make_async_copy(mass_hbm, mass_ref, load_sems.at[parts + 4]),
    ]
    for item in small:
        item.start()

    barrier = pltpu.get_barrier_semaphore()
    for place in range(n - 1):
        pl.semaphore_signal(barrier, inc=1, device_id=(peer[place],), device_id_type=MESH)

    loads = []
    for part in range(parts):
        span = pl.ds(part * chunk, chunk)
        loads.append(
            pltpu.make_async_copy(coup_hbm.at[span], coup.at[span], load_sems.at[part])
        )
    loads.append(pltpu.make_async_copy(diag_hbm, diag, load_sems.at[parts]))
    for item in loads:
        item.start()
    for item in small:
        item.wait()

    rows = rows_ref[...]
    cols = cols_ref[...]
    low = me * rb
    pushes = (rows < low) | (rows >= low + rb)
    push_l = jnp.where(pushes, 1, 0)
    rem_l = jnp.where(pushes, rows, cols)
    loc_l = jnp.where(pushes, cols, rows) - low
    own_l = (rem_l * (-(-65536 // rb))) >> 16
    far_l = rem_l - own_l * rb
    square = (tiles, tiles)
    eye = iota(square, 0) == iota(square, 1)
    earlier = iota(square, 0) < iota(square, 1)

    def to_s(value, zero):
        return jnp.sum(jnp.where(eye, value, zero), axis=1, keepdims=True)

    key_l = own_l + push_l * n
    key_s = to_s(key_l, 0)
    slot_l = jnp.sum(jnp.where((key_s == key_l) & earlier, 1, 0), axis=0, keepdims=True)
    line_l = (n - 1 - (own_l ^ me)) * slots + slot_l
    tile_l = iota((1, tiles), 1)
    line_s = to_s(line_l + push_l * lanes, 0)
    pack_s = to_s(((tile_l * BASE + loc_l) * BASE + far_l) + 1, 0)
    name_s = to_s(own_l * slots + slot_l, 0)
    code_s = to_s(jnp.where(pushes, (far_l + 1) * BASE, far_l + 1).astype(F32), 0.0)
    wide = (tiles, lanes)
    lane_w = iota(wide, 1)
    kinds = []
    for kind in range(2):
        here = line_s == lane_w + kind * lanes
        packed = jnp.sum(jnp.where(here, pack_s, 0), axis=0, keepdims=True)
        there = packed > 0
        packed = jnp.where(there, packed - 1, 0)
        local = jnp.clip((packed >> 6) & (BASE - 1), 0, rb - 1)
        kinds.append(jnp.clip(packed >> 12, 0, tiles - 1))
        kinds.append(jnp.where(there, local, BASE) if kind == 0 else local)
        if kind == 0:
            kinds.append(jnp.clip(packed & (BASE - 1), 0, rb - 1))
    for index, value in enumerate(kinds):
        table_v[index : index + 1, :] = value
    table_copy = pltpu.make_async_copy(table_v, table, table_sem)
    table_copy.start()
    code = jnp.sum(jnp.where(name_s == lane_w, code_s, 0.0), axis=0, keepdims=True)
    code = code[:, 0:128]

    wbuf[...] = jnp.zeros(wbuf.shape, F32)
    wbuf[0:rb, :] = -defect_ref[...]
    vector = wbuf[...]
    lane_1 = iota((1, 128), 1)
    code = jnp.where(lane_1 == me * slots, total(vector * vector), code)
    send0[0:rb, 0, :] = -defect_ref[...]
    send0[rb, :, :] = code
    codes[n - 1 : n, :] = code

    pl.semaphore_wait(barrier, n - 1)

    def send(phase, group, source, target, size, spread):
        for place in range(*groups[group]):
            span = pl.ds(place * size, size)
            pltpu.make_async_remote_copy(
                src_ref=source.at[span] if spread else source,
                dst_ref=target.at[span],
                send_sem=sent.at[phase],
                recv_sem=got.at[phase, group],
                device_id=(peer[place],),
                device_id_type=MESH,
            ).start()

    def await_group(phase, group, target, size):
        first, last = groups[group]
        view = target.at[pl.ds(first * size, (last - first) * size)]
        pltpu.make_async_copy(view, view, got.at[phase, group]).wait()

    def await_sent(phase, target, size):
        view = target.at[pl.ds(0, (n - 1) * size)]
        pltpu.make_async_copy(view, view, sent.at[phase]).wait()

    for group in range(count):
        send(0, group, send0, recv0, head, False)

    lane_k = iota((width, 128), 1)
    sub = iota((pad, 128), 0)
    sub_f = sub.astype(F32)
    empty = jnp.zeros((width, 128), F32)

    def slots_of(group):
        first, last = groups[group]
        return [(place, slot) for place in range(first, last) for slot in range(slots)]

    def product(tile, row):
        return jnp.sum(tile * row, axis=1, keepdims=True)

    def push_sums(group):
        acc = empty
        for index, (place, slot) in enumerate(slots_of(group)):
            line = place * slots + slot
            row = wbuf[pl.ds(table[4, line], 1), :]
            acc = jnp.where(lane_k == index, product(coup[table[3, line]], row), acc)
        return acc

    def push_out(turn, group, acc):
        found = acc.T
        for index, (place, slot) in enumerate(slots_of(group)):
            send_b[turn, place * slots + slot, :, :] = found[index : index + 1, :]
        send(1 + 2 * turn, group, send_b.at[turn], recv_b.at[turn], slots, True)

    def push_all(turn):
        held = push_sums(0)
        for group in range(count):
            later = push_sums(group + 1) if group + 1 < count else None
            push_out(turn, group, held)
            held = later

    def fetch_sums(group, source):
        acc = empty
        for index, (place, slot) in enumerate(slots_of(group)):
            line = place * slots + slot
            row = source(place, slot)
            acc = jnp.where(lane_k == index, product(coup[table[0, line]], row), acc)
        return acc

    def fetch_in(group, image, acc):
        found = acc.T
        for index, (place, slot) in enumerate(slots_of(group)):
            here = sub == table[1, place * slots + slot]
            image = image + jnp.where(here, found[index : index + 1, :], 0.0)
        return image

    def fetch_all(image, ready, source):
        held = None
        for group in near_first:
            ready(group)
            sums = fetch_sums(group, source)
            if held is not None:
                image = fetch_in(group + 1, image, held)
            held = sums
        return fetch_in(0, image, held)

    def own_rows(image):
        acc = empty
        for index in range(rb):
            value = product(diag[index], wbuf[index : index + 1, :])
            acc = jnp.where(lane_k == index, value, acc)
        return image + acc.T[0:pad, :]

    def land_group(turn, group, image):
        for place, slot in slots_of(group):
            here = goal_ref[slot, place : place + 1, :] == sub_f
            line = recv_b[turn, place * slots + slot, :, :]
            image = image + jnp.where(here, line, 0.0)
        return image

    def decode(first, last):
        shape = (last - first, 128)
        found = codes[first:last, :]
        lane = iota(shape, 1)
        for slot in range(slots):
            mine = jnp.where(lane == me * slots + slot, found, 0.0)
            value = jnp.sum(mine, axis=1, keepdims=True)
            goal = jnp.floor(value * (1.0 / BASE))
            goal_ref[slot, first:last, :] = jnp.broadcast_to(goal - 1.0, shape)
            ask_ref[slot, first:last, :] = jnp.broadcast_to(value - goal * BASE - 1.0, shape)

    def gather_group(turn, group, vector):
        for place, slot in slots_of(group):
            here = ask_ref[slot, place : place + 1, :] == sub_f
            line = jnp.sum(jnp.where(here, vector, 0.0), axis=0, keepdims=True)
            send_a[turn - 1, place * lines + slot, :, :] = line

    def send_asked(turn, group, own_part):
        for place in range(*groups[group]):
            send_a[turn - 1, place * lines + slots, :, :] = own_part
        send(2 * turn, group, send_a.at[turn - 1], recv_a.at[turn - 1], lines, True)

    for item in loads:
        item.wait()
    table_copy.wait()
    mass = jnp.concatenate([mass_ref[...], jnp.zeros((pad - rb, 128), F32)], axis=0)

    near_first = list(reversed(range(count)))
    push_all(0)
    image = own_rows(mass * vector)

    def ready_first(group):
        await_group(0, group, recv0, head)
        for place in range(*groups[group]):
            codes[place : place + 1, :] = recv0[place * head + rb]
            for row in range(rb):
                blocks[place * rb + row, :, :] = recv0[place * head + row]

    def block_row(place, slot):
        return blocks[place * rb + table[2, place * slots + slot]]

    image = fetch_all(image, ready_first, block_row)
    decode(0, n)
    whose = (n - 1 - iota((n, 128), 0)) ^ me
    squares = total(jnp.where(iota((n, 128), 1) == whose * slots, codes[...], 0.0))
    beta = jnp.sqrt(squares)
    for group in near_first:
        await_group(1, group, recv_b.at[0], slots)
        image = land_group(0, group, image)
    basis = [vector / beta]
    images = [image / beta]
    heads = []
    gram = {}

    for turn in range(1, ITERS):
        vector = images[-1]
        wbuf[...] = vector
        own_part = as_row(
            [total(vector * item) for item in basis]
            + [total(vector * item) for item in images]
        )
        for group in range(count):
            gather_group(turn, group, vector)
            send_asked(turn, group, own_part)
        push_all(turn)
        image = own_rows(mass * vector)
        parts_of = [own_part]

        def ready(group):
            await_group(2 * turn, group, recv_a.at[turn - 1], lines)
            for place in range(*groups[group]):
                parts_of.append(recv_a[turn - 1, place * lines + slots, :, :])

        def asked_row(place, slot):
            return recv_a[turn - 1, place * lines + slot, :, :]

        image = fetch_all(image, ready, asked_row)
        sums = sum(parts_of[1:], parts_of[0])
        dots = [pick(sums, index) for index in range(turn)]
        for index in range(turn):
            gram[index, turn - 1] = pick(sums, turn + index)
        heads.append(dots[0])
        square = gram[turn - 1, turn - 1]
        left = square
        for value in dots:
            left = left - value * value
        scale = lax.rsqrt(jnp.maximum(left, square * 1e-6))
        for index in range(turn):
            vector = vector - dots[index] * basis[index]
        basis.append(vector * scale)
        for group in near_first:
            await_group(1 + 2 * turn, group, recv_b.at[turn], slots)
            image = land_group(turn, group, image)
        for index in range(turn):
            image = image - dots[index] * images[index]
        images.append(image * scale)

    vector = images[-1]
    own_part = as_row(
        [total(vector * basis[0])] + [total(vector * item) for item in images]
    )
    send_f[0] = own_part
    last_phase = 2 * ITERS
    for group in range(count):
        send(last_phase, group, send_f, recv_f, 1, False)
    sums = own_part
    for group in near_first:
        await_group(last_phase, group, recv_f, 1)
        for place in range(*groups[group]):
            sums = sums + recv_f[place, :, :]
    heads.append(pick(sums, 0))
    for index in range(ITERS):
        gram[index, ITERS - 1] = pick(sums, 1 + index)

    factor = {}
    for i in range(ITERS):
        for j in range(i + 1):
            value = gram[j, i]
            for k in range(j):
                value = value - factor[i, k] * factor[j, k]
            factor[i, j] = jnp.sqrt(value) if i == j else value / factor[j, j]
    forward = []
    for i in range(ITERS):
        value = beta * heads[i]
        for k in range(i):
            value = value - factor[i, k] * forward[k]
        forward.append(value / factor[i, i])
    mixing = [None] * ITERS
    for i in reversed(range(ITERS)):
        value = forward[i]
        for k in range(i + 1, ITERS):
            value = value - factor[k, i] * mixing[k]
        mixing[i] = value / factor[i, i]
    update = mixing[0] * basis[0]
    for i in range(1, ITERS):
        update = update + mixing[i] * basis[i]
    out_ref[...] = update[0:rb, :]

    await_sent(0, recv0, head)
    for turn in range(ITERS):
        await_sent(1 + 2 * turn, recv_b.at[turn], slots)
    for turn in range(1, ITERS):
        await_sent(2 * turn, recv_a.at[turn - 1], lines)
    await_sent(last_phase, recv_f, 1)


def on_device(defect, mass, block_diag, coupling, tile_rows, tile_cols):
    rb, width = defect.shape
    tiles = tile_rows.shape[0]
    n = lax.axis_size("blk")
    slots = (tiles // 2 + n - 2) // (n - 1)
    lines = slots + 1
    pad = -(-rb // 8) * 8
    lanes = -(-n * slots // 128) * 128
    hbm = pl.BlockSpec(memory_space=pltpu.HBM)
    phases = 2 * ITERS + 1
    return pl.pallas_call(
        functools.partial(kernel, n, slots),
        out_shape=jax.ShapeDtypeStruct((rb, width), F32),
        in_specs=[hbm] * 6,
        out_specs=pl.BlockSpec(memory_space=pltpu.VMEM),
        scratch_shapes=[
            pltpu.VMEM((tiles, width, width), F32),
            pltpu.VMEM((rb, width, width), F32),
            pltpu.VMEM((rb, width), F32),
            pltpu.VMEM((rb, width), F32),
            pltpu.VMEM((1, tiles), I32),
            pltpu.VMEM((1, tiles), I32),
            pltpu.VMEM((8, lanes), I32),
            pltpu.SMEM((8, lanes), I32),
            pltpu.VMEM((pad, width), F32),
            pltpu.VMEM((n, width), F32),
            pltpu.VMEM((slots, n, width), F32),
            pltpu.VMEM((slots, n, width), F32),
            pltpu.VMEM((rb + 1, 1, width), F32),
            pltpu.VMEM((n * (rb + 1), 1, width), F32),
            pltpu.VMEM((n * rb, 1, width), F32),
            pltpu.VMEM((ITERS - 1, n * lines, 1, width), F32),
            pltpu.VMEM((ITERS - 1, n * lines, 1, width), F32),
            pltpu.VMEM((ITERS, n * slots, 1, width), F32),
            pltpu.VMEM((ITERS, n * slots, 1, width), F32),
            pltpu.VMEM((1, 1, width), F32),
            pltpu.VMEM((n, 1, width), F32),
            pltpu.SemaphoreType.DMA((9,)),
            pltpu.SemaphoreType.DMA,
            pltpu.SemaphoreType.DMA((phases,)),
            pltpu.SemaphoreType.DMA((phases, len(ranges(n)))),
        ],
        compiler_params=pltpu.CompilerParams(
            collective_id=0, has_side_effects=True, vmem_limit_bytes=VMEM_LIMIT
        ),
    )(
        defect,
        mass,
        block_diag,
        coupling,
        tile_rows.reshape(1, tiles),
        tile_cols.reshape(1, tiles),
    )


def solution(mesh):
    in_specs = (
        P("blk", None),
        P("blk", None),
        P("blk", None, None),
        P("blk", None, None),
        P("blk"),
        P("blk"),
    )
    return jax.shard_map(
        on_device, mesh=mesh, in_specs=in_specs, out_specs=P("blk", None), check_vma=False
    )
```

```python
import functools

import jax
import jax.numpy as jnp
from jax import lax
from jax.experimental import pallas as pl
from jax.experimental.pallas import tpu as pltpu
from jax.sharding import PartitionSpec as P

ITERS = 3
F32 = jnp.float32
I32 = jnp.int32
MESH = pl.DeviceIdType.MESH
BASE = 64
VMEM_LIMIT = 57 * 1024 * 1024


def iota(shape, axis):
    return lax.broadcasted_iota(I32, shape, axis)


def iota_f(shape, axis):
    return iota(shape, axis).astype(F32)


def total(value):
    return jnp.sum(jnp.sum(value, axis=0, keepdims=True), axis=1, keepdims=True)


def as_row(items):
    lane = iota((1, 128), 1)
    row = jnp.zeros((1, 128), F32)
    for index, item in enumerate(items):
        row = jnp.where(lane == index, item, row)
    return row


def pick(row, index):
    lane = iota((1, 128), 1)
    return jnp.sum(jnp.where(lane == index, row, 0.0), axis=1, keepdims=True)


def ranges(n):
    cuts = [0, 2, 6, 10, n // 2, n - n // 4, n - 1]
    cuts = sorted({min(cut, n - 1) for cut in cuts})
    return list(zip(cuts[:-1], cuts[1:]))


def kernel(
    n,
    slots,
    defect_hbm,
    mass_hbm,
    diag_hbm,
    coup_hbm,
    rows_hbm,
    cols_hbm,
    out_ref,
    coup,
    diag,
    defect_ref,
    mass_ref,
    rows_ref,
    cols_ref,
    table_v,
    table,
    wbuf,
    held,
    far_t,
    diag_t,
    codes,
    ask_ref,
    goal_ref,
    send0,
    recv0,
    blocks,
    send_a,
    recv_a,
    send_b,
    recv_b,
    send_f,
    recv_f,
    load_sems,
    table_sem,
    sent,
    passed,
    got,
):
    me = lax.axis_index("blk")
    rb, width = defect_ref.shape
    tiles = rows_ref.shape[1]
    pad = wbuf.shape[0]
    lanes = table.shape[1]
    parts = 4
    chunk = tiles // parts
    groups = ranges(n)
    count = len(groups)
    head = rb + 1
    lines = slots + 1

    peers = {0: me}
    for mask in range(1, n):
        low_bit = mask & -mask
        sign = 1 - 2 * ((me // low_bit) % 2)
        peers[mask] = peers[mask - low_bit] + sign * low_bit
    peer = [peers[n - 1 - place] for place in range(n)]

    small = [
        pltpu.make_async_copy(rows_hbm, rows_ref, load_sems.at[parts + 1]),
        pltpu.make_async_copy(cols_hbm, cols_ref, load_sems.at[parts + 2]),
        pltpu.make_async_copy(defect_hbm, defect_ref, load_sems.at[parts + 3]),
        pltpu.make_async_copy(mass_hbm, mass_ref, load_sems.at[parts + 4]),
    ]
    for item in small:
        item.start()

    barrier = pltpu.get_barrier_semaphore()
    for place in range(n - 1):
        pl.semaphore_signal(barrier, inc=1, device_id=(peer[place],), device_id_type=MESH)

    loads = []
    for part in range(parts):
        span = pl.ds(part * chunk, chunk)
        loads.append(
            pltpu.make_async_copy(coup_hbm.at[span], coup.at[span], load_sems.at[part])
        )
    loads.append(pltpu.make_async_copy(diag_hbm, diag, load_sems.at[parts]))
    for item in loads:
        item.start()
    for item in small:
        item.wait()

    rows = rows_ref[...]
    cols = cols_ref[...]
    low = me * rb
    pushes = (rows < low) | (rows >= low + rb)
    push_l = jnp.where(pushes, 1, 0)
    rem_l = jnp.where(pushes, rows, cols)
    loc_l = jnp.where(pushes, cols, rows) - low
    own_l = (rem_l * (-(-65536 // rb))) >> 16
    far_l = rem_l - own_l * rb
    square = (tiles, tiles)
    eye = iota(square, 0) == iota(square, 1)
    earlier = iota(square, 0) < iota(square, 1)

    def to_s(value, zero):
        return jnp.sum(jnp.where(eye, value, zero), axis=1, keepdims=True)

    key_l = own_l + push_l * n
    key_s = to_s(key_l, 0)
    slot_l = jnp.sum(jnp.where((key_s == key_l) & earlier, 1, 0), axis=0, keepdims=True)
    line_l = (n - 1 - (own_l ^ me)) * slots + slot_l
    tile_l = iota((1, tiles), 1)
    line_s = to_s(line_l + push_l * lanes, 0)
    pack_s = to_s(((tile_l * BASE + loc_l) * BASE + far_l) + 1, 0)
    name_s = to_s(own_l * slots + slot_l, 0)
    code_s = to_s(jnp.where(pushes, (far_l + 1) * BASE, far_l + 1).astype(F32), 0.0)
    wide = (tiles, lanes)
    lane_w = iota(wide, 1)
    kinds = []
    for kind in range(2):
        here = line_s == lane_w + kind * lanes
        packed = jnp.sum(jnp.where(here, pack_s, 0), axis=0, keepdims=True)
        there = packed > 0
        packed = jnp.where(there, packed - 1, 0)
        local = jnp.clip((packed >> 6) & (BASE - 1), 0, rb - 1)
        kinds.append(jnp.clip(packed >> 12, 0, tiles - 1))
        kinds.append(jnp.where(there, local, BASE) if kind == 0 else local)
        if kind == 0:
            kinds.append(jnp.clip(packed & (BASE - 1), 0, rb - 1))
    for index, value in enumerate(kinds):
        table_v[index : index + 1, :] = value
    table_copy = pltpu.make_async_copy(table_v, table, table_sem)
    table_copy.start()
    code = jnp.sum(jnp.where(name_s == lane_w, code_s, 0.0), axis=0, keepdims=True)
    code = code[:, 0:128]

    wbuf[...] = jnp.zeros(wbuf.shape, F32)
    wbuf[0:rb, :] = -defect_ref[...]
    vector = wbuf[...]
    lane_1 = iota((1, 128), 1)
    code = jnp.where(lane_1 == me * slots, total(vector * vector), code)
    send0[0:rb, 0, :] = -defect_ref[...]
    send0[rb, :, :] = code
    codes[n - 1 : n, :] = code

    pl.semaphore_wait(barrier, n - 1)

    def send(phase, group, source, target, size, spread):
        for place in range(*groups[group]):
            span = pl.ds(place * size, size)
            pltpu.make_async_remote_copy(
                src_ref=source.at[span] if spread else source,
                dst_ref=target.at[span],
                send_sem=sent.at[phase],
                recv_sem=got.at[phase, group],
                device_id=(peer[place],),
                device_id_type=MESH,
            ).start()

    def await_group(phase, group, target, size):
        first, last = groups[group]
        view = target.at[pl.ds(first * size, (last - first) * size)]
        pltpu.make_async_copy(view, view, got.at[phase, group]).wait()

    def await_sent(phase, target, size):
        view = target.at[pl.ds(0, (n - 1) * size)]
        pltpu.make_async_copy(view, view, sent.at[phase]).wait()

    core = me % 2

    def first_copy(source, group, device, spot, size, sem):
        return pltpu.make_async_remote_copy(
            src_ref=source,
            dst_ref=recv0.at[pl.ds(spot * head, size * head)],
            send_sem=sem,
            recv_sem=got.at[0, group],
            device_id=(device,),
            device_id_type=MESH,
        )

    for group in range(count):
        for place in range(groups[group][0], groups[group][1], 2):
            if place < n - 2:
                device, spot = peer[place + 1] + 1 - core, place + core
            else:
                device, spot = peer[place], place
            first_copy(send0, group, device, spot, 1, sent.at[0]).start()

    def pass_on(group):
        first, last = groups[group]
        last = min(last, n - 2)
        part = recv0.at[pl.ds(first * head, (last - first) * head)]
        return first_copy(part, group, peer[n - 2], first, last - first, passed)

    lane_k = iota((width, 128), 1)
    sub = iota((pad, 128), 0)
    sub_f = sub.astype(F32)
    empty = jnp.zeros((width, 128), F32)

    def slots_of(group):
        first, last = groups[group]
        return [(place, slot) for place in range(first, last) for slot in range(slots)]

    def product(tile, row):
        return jnp.sum(tile * row, axis=1, keepdims=True)

    def spread(vector):
        wbuf[...] = vector
        filled = jnp.concatenate([vector, jnp.zeros((width - pad, 128), F32)], axis=0)
        turned = filled.T
        for index in range(rb):
            held[index] = jnp.broadcast_to(turned[:, index : index + 1], (width, 128))

    def push_group(turn, group):
        for place, slot in slots_of(group):
            line = place * slots + slot
            value = far_t[line] * held[table[4, line]]
            send_b[turn, line, :, :] = jnp.sum(value, axis=0, keepdims=True)
        send(1 + 2 * turn, group, send_b.at[turn], recv_b.at[turn], slots, True)

    def own_rows(image):
        for index in range(rb):
            value = jnp.sum(diag_t[index] * held[index], axis=0, keepdims=True)
            image = image + jnp.where(sub == index, value, 0.0)
        return image

    def fetch_all(image, ready, source, between):
        acc = empty
        for group in near_first:
            ready(group)
            for place, slot in slots_of(group):
                line = place * slots + slot
                value = product(coup[table[0, line]], source(place, slot))
                acc = acc + jnp.where(lane_k == table[1, line], value, 0.0)
            image = between(group, image)
        return image + acc.T[0:pad, :]

    def land_group(turn, group, image):
        for place, slot in slots_of(group):
            here = goal_ref[slot, place : place + 1, :] == sub_f
            line = recv_b[turn, place * slots + slot, :, :]
            image = image + jnp.where(here, line, 0.0)
        return image

    def decode(first, last):
        shape = (last - first, 128)
        found = codes[first:last, :]
        lane = iota(shape, 1)
        for slot in range(slots):
            mine = jnp.where(lane == me * slots + slot, found, 0.0)
            value = jnp.sum(mine, axis=1, keepdims=True)
            goal = jnp.floor(value * (1.0 / BASE))
            goal_ref[slot, first:last, :] = jnp.broadcast_to(goal - 1.0, shape)
            ask_ref[slot, first:last, :] = jnp.broadcast_to(value - goal * BASE - 1.0, shape)

    def gather_group(turn, group, vector):
        for place, slot in slots_of(group):
            here = ask_ref[slot, place : place + 1, :] == sub_f
            line = jnp.sum(jnp.where(here, vector, 0.0), axis=0, keepdims=True)
            send_a[turn - 1, place * lines + slot, :, :] = line

    def send_asked(turn, group, own_part):
        for place in range(*groups[group]):
            send_a[turn - 1, place * lines + slots, :, :] = own_part
        send(2 * turn, group, send_a.at[turn - 1], recv_a.at[turn - 1], lines, True)

    for item in loads:
        item.wait()
    table_copy.wait()
    mass = jnp.concatenate([mass_ref[...], jnp.zeros((pad - rb, 128), F32)], axis=0)

    urgent = [group for group in range(count) if groups[group][0] < 8]
    early = [group for group in reversed(range(count)) if groups[group][0] >= 8]
    near_first = list(reversed(range(count)))
    spread(vector)
    for group in range(count):
        for place, slot in slots_of(group):
            line = place * slots + slot
            far_t[line] = coup[table[3, line]].T
        push_group(0, group)
    for index in range(rb):
        diag_t[index] = diag[index].T
    image = own_rows(mass * vector)
    landed = {2: near_first[:2], 1: near_first[2:-2]} if count > 4 else {1: near_first[:-2]}

    def ready_first(group):
        await_group(0, group, recv0, head)
        pl.when(core == 1)(pass_on(group).start)
        for place in range(*groups[group]):
            spot = place
            if place < n - 2:
                spot = place + (1 - core) * (1 - 2 * (place % 2))
            codes[place : place + 1, :] = recv0[spot * head + rb]
            for row in range(rb):
                blocks[place * rb + row, :, :] = recv0[spot * head + row]

    def block_row(place, slot):
        return blocks[place * rb + table[2, place * slots + slot]]

    def between_first(group, image):
        if group == 1:
            decode(8, n)
            for other in early:
                await_group(1, other, recv_b.at[0], slots)
                image = land_group(0, other, image)
        return image

    image = fetch_all(image, ready_first, block_row, between_first)
    decode(0, 8)
    whose = (n - 1 - iota((n, 128), 0)) ^ me
    squares = total(jnp.where(iota((n, 128), 1) == whose * slots, codes[...], 0.0))
    beta = jnp.sqrt(squares)
    for group in near_first:
        if group in early:
            continue
        await_group(1, group, recv_b.at[0], slots)
        image = land_group(0, group, image)
    basis = [vector / beta]
    images = [image / beta]
    heads = []
    gram = {}

    for turn in range(1, ITERS):
        vector = images[-1]
        own_part = as_row(
            [total(vector * item) for item in basis]
            + [total(vector * item) for item in images]
        )
        for group in urgent:
            gather_group(turn, group, vector)
            send_asked(turn, group, own_part)
        spread(vector)
        for group in urgent:
            push_group(turn, group)
        for group in range(len(urgent), count):
            gather_group(turn, group, vector)
            send_asked(turn, group, own_part)
        for group in range(len(urgent), count):
            push_group(turn, group)
        image = own_rows(mass * vector)
        parts_of = [own_part]

        def ready(group):
            await_group(2 * turn, group, recv_a.at[turn - 1], lines)
            for place in range(*groups[group]):
                parts_of.append(recv_a[turn - 1, place * lines + slots, :, :])

        def asked_row(place, slot):
            return recv_a[turn - 1, place * lines + slot, :, :]

        def between(group, image):
            for other in landed.get(group, ()):
                await_group(1 + 2 * turn, other, recv_b.at[turn], slots)
                image = land_group(turn, other, image)
            return image

        image = fetch_all(image, ready, asked_row, between)
        sums = sum(parts_of[1:], parts_of[0])
        dots = [pick(sums, index) for index in range(turn)]
        for index in range(turn):
            gram[index, turn - 1] = pick(sums, turn + index)
        heads.append(dots[0])
        square = gram[turn - 1, turn - 1]
        left = square
        for value in dots:
            left = left - value * value
        scale = lax.rsqrt(jnp.maximum(left, square * 1e-6))
        for index in range(turn):
            vector = vector - dots[index] * basis[index]
        basis.append(vector * scale)
        for group in near_first[-2:]:
            await_group(1 + 2 * turn, group, recv_b.at[turn], slots)
            image = land_group(turn, group, image)
        for index in range(turn):
            image = image - dots[index] * images[index]
        images.append(image * scale)

    vector = images[-1]
    own_part = as_row(
        [total(vector * basis[0])] + [total(vector * item) for item in images]
    )
    send_f[0] = own_part
    last_phase = 2 * ITERS
    for group in range(count):
        send(last_phase, group, send_f, recv_f, 1, False)
    sums = own_part
    for group in near_first:
        await_group(last_phase, group, recv_f, 1)
        for place in range(*groups[group]):
            sums = sums + recv_f[place, :, :]
    heads.append(pick(sums, 0))
    for index in range(ITERS):
        gram[index, ITERS - 1] = pick(sums, 1 + index)

    factor = {}
    for i in range(ITERS):
        for j in range(i + 1):
            value = gram[j, i]
            for k in range(j):
                value = value - factor[i, k] * factor[j, k]
            factor[i, j] = jnp.sqrt(value) if i == j else value / factor[j, j]
    forward = []
    for i in range(ITERS):
        value = beta * heads[i]
        for k in range(i):
            value = value - factor[i, k] * forward[k]
        forward.append(value / factor[i, i])
    mixing = [None] * ITERS
    for i in reversed(range(ITERS)):
        value = forward[i]
        for k in range(i + 1, ITERS):
            value = value - factor[k, i] * mixing[k]
        mixing[i] = value / factor[i, i]
    update = mixing[0] * basis[0]
    for i in range(1, ITERS):
        update = update + mixing[i] * basis[i]
    out_ref[...] = update[0:rb, :]

    view = recv0.at[pl.ds(0, n // 2 * head)]
    pltpu.make_async_copy(view, view, sent.at[0]).wait()
    whole = recv0.at[pl.ds(0, (n - 2) * head)]
    pl.when(core == 1)(pltpu.make_async_copy(whole, whole, passed).wait)
    for turn in range(ITERS):
        await_sent(1 + 2 * turn, recv_b.at[turn], slots)
    for turn in range(1, ITERS):
        await_sent(2 * turn, recv_a.at[turn - 1], lines)
    await_sent(last_phase, recv_f, 1)


def on_device(defect, mass, block_diag, coupling, tile_rows, tile_cols):
    rb, width = defect.shape
    tiles = tile_rows.shape[0]
    n = lax.axis_size("blk")
    slots = (tiles // 2 + n - 2) // (n - 1)
    lines = slots + 1
    pad = -(-rb // 8) * 8
    lanes = -(-n * slots // 128) * 128
    hbm = pl.BlockSpec(memory_space=pltpu.HBM)
    phases = 2 * ITERS + 1
    return pl.pallas_call(
        functools.partial(kernel, n, slots),
        out_shape=pltpu.VMEM((rb, width), F32),
        in_specs=[hbm] * 6,
        out_specs=pl.BlockSpec(memory_space=pltpu.VMEM),
        scratch_shapes=[
            pltpu.VMEM((tiles, width, width), F32),
            pltpu.VMEM((rb, width, width), F32),
            pltpu.VMEM((rb, width), F32),
            pltpu.VMEM((rb, width), F32),
            pltpu.VMEM((1, tiles), I32),
            pltpu.VMEM((1, tiles), I32),
            pltpu.VMEM((8, lanes), I32),
            pltpu.SMEM((8, lanes), I32),
            pltpu.VMEM((pad, width), F32),
            pltpu.VMEM((rb, width, width), F32),
            pltpu.VMEM(((n - 1) * slots, width, width), F32),
            pltpu.VMEM((rb, width, width), F32),
            pltpu.VMEM((n, width), F32),
            pltpu.VMEM((slots, n, width), F32),
            pltpu.VMEM((slots, n, width), F32),
            pltpu.VMEM((rb + 1, 1, width), F32),
            pltpu.VMEM((n * (rb + 1), 1, width), F32),
            pltpu.VMEM((n * rb, 1, width), F32),
            pltpu.VMEM((ITERS - 1, n * lines, 1, width), F32),
            pltpu.VMEM((ITERS - 1, n * lines, 1, width), F32),
            pltpu.VMEM((ITERS, n * slots, 1, width), F32),
            pltpu.VMEM((ITERS, n * slots, 1, width), F32),
            pltpu.VMEM((1, 1, width), F32),
            pltpu.VMEM((n, 1, width), F32),
            pltpu.SemaphoreType.DMA((9,)),
            pltpu.SemaphoreType.DMA,
            pltpu.SemaphoreType.DMA((phases,)),
            pltpu.SemaphoreType.DMA,
            pltpu.SemaphoreType.DMA((phases, len(ranges(n)))),
        ],
        compiler_params=pltpu.CompilerParams(
            collective_id=0, has_side_effects=True, vmem_limit_bytes=VMEM_LIMIT
        ),
    )(
        defect,
        mass,
        block_diag,
        coupling,
        tile_rows.reshape(1, tiles),
        tile_cols.reshape(1, tiles),
    )


def solution(mesh):
    in_specs = (
        P("blk", None),
        P("blk", None),
        P("blk", None, None),
        P("blk", None, None),
        P("blk"),
        P("blk"),
    )
    return jax.shard_map(
        on_device, mesh=mesh, in_specs=in_specs, out_specs=P("blk", None), check_vma=False
    )
```

```python
import functools

import jax
import jax.numpy as jnp
from jax import lax
from jax.experimental import pallas as pl
from jax.experimental.pallas import tpu as pltpu
from jax.sharding import PartitionSpec as P

ITERS = 3
F32 = jnp.float32
I32 = jnp.int32
MESH = pl.DeviceIdType.MESH
BASE = 64
VMEM_LIMIT = 57 * 1024 * 1024


def iota(shape, axis):
    return lax.broadcasted_iota(I32, shape, axis)


def iota_f(shape, axis):
    return iota(shape, axis).astype(F32)


def total(value):
    return jnp.sum(jnp.sum(value, axis=0, keepdims=True), axis=1, keepdims=True)


def as_row(items):
    lane = iota((1, 128), 1)
    row = jnp.zeros((1, 128), F32)
    for index, item in enumerate(items):
        row = jnp.where(lane == index, item, row)
    return row


def pick(row, index):
    lane = iota((1, 128), 1)
    return jnp.sum(jnp.where(lane == index, row, 0.0), axis=1, keepdims=True)


def layout(n):
    def far(chip):
        return min((chip & 1) + (chip >> 1 & 1) + (chip >> 2), 5)

    chips = sorted(range(n // 2), key=lambda chip: (-far(chip), -chip))
    masks = [2 * chip + bit for chip in chips for bit in (1, 0)]
    levels = [max(far(mask // 2), 1) for mask in masks[: n - 1]]
    starts = [at for at in range(n - 1) if at == 0 or levels[at] != levels[at - 1]]
    return masks, list(zip(starts, starts[1:] + [n - 1]))


def kernel(
    n,
    slots,
    defect_hbm,
    mass_hbm,
    diag_hbm,
    coup_hbm,
    rows_hbm,
    cols_hbm,
    out_ref,
    coup,
    diag,
    defect_ref,
    mass_ref,
    rows_ref,
    cols_ref,
    table_v,
    table,
    wbuf,
    held,
    far_t,
    diag_t,
    codes,
    ask_ref,
    goal_ref,
    send0,
    recv0,
    blocks,
    send_a,
    recv_a,
    send_b,
    recv_b,
    send_f,
    recv_f,
    load_sems,
    table_sem,
    sent,
    passed,
    got,
):
    me = lax.axis_index("blk")
    rb, width = defect_ref.shape
    tiles = rows_ref.shape[1]
    pad = wbuf.shape[0]
    lanes = table.shape[1]
    parts = 4
    chunk = tiles // parts
    masks, groups = layout(n)
    count = len(groups)
    head = rb + 1
    lines = slots + 1

    peers = {0: me}
    for mask in range(1, n):
        low_bit = mask & -mask
        sign = 1 - 2 * ((me // low_bit) % 2)
        peers[mask] = peers[mask - low_bit] + sign * low_bit
    peer = [peers[mask] for mask in masks]

    small = [
        pltpu.make_async_copy(rows_hbm, rows_ref, load_sems.at[parts + 1]),
        pltpu.make_async_copy(cols_hbm, cols_ref, load_sems.at[parts + 2]),
        pltpu.make_async_copy(defect_hbm, defect_ref, load_sems.at[parts + 3]),
        pltpu.make_async_copy(mass_hbm, mass_ref, load_sems.at[parts + 4]),
    ]
    for item in small:
        item.start()

    barrier = pltpu.get_barrier_semaphore()
    for place in range(n - 1):
        pl.semaphore_signal(barrier, inc=1, device_id=(peer[place],), device_id_type=MESH)

    loads = []
    for part in range(parts):
        span = pl.ds(part * chunk, chunk)
        loads.append(
            pltpu.make_async_copy(coup_hbm.at[span], coup.at[span], load_sems.at[part])
        )
    loads.append(pltpu.make_async_copy(diag_hbm, diag, load_sems.at[parts]))
    for item in loads:
        item.start()
    for item in small:
        item.wait()

    rows = rows_ref[...]
    cols = cols_ref[...]
    low = me * rb
    pushes = (rows < low) | (rows >= low + rb)
    push_l = jnp.where(pushes, 1, 0)
    rem_l = jnp.where(pushes, rows, cols)
    loc_l = jnp.where(pushes, cols, rows) - low
    own_l = (rem_l * (-(-65536 // rb))) >> 16
    far_l = rem_l - own_l * rb
    square = (tiles, tiles)
    eye = iota(square, 0) == iota(square, 1)
    earlier = iota(square, 0) < iota(square, 1)

    def to_s(value, zero):
        return jnp.sum(jnp.where(eye, value, zero), axis=1, keepdims=True)

    key_l = own_l + push_l * n
    key_s = to_s(key_l, 0)
    slot_l = jnp.sum(jnp.where((key_s == key_l) & earlier, 1, 0), axis=0, keepdims=True)
    apart = own_l ^ me
    place_l = sum(jnp.where(apart == mask, at, 0) for at, mask in enumerate(masks))
    line_l = place_l * slots + slot_l
    tile_l = iota((1, tiles), 1)
    line_s = to_s(line_l + push_l * lanes, 0)
    pack_s = to_s(((tile_l * BASE + loc_l) * BASE + far_l) + 1, 0)
    name_s = to_s(own_l * slots + slot_l, 0)
    code_s = to_s(jnp.where(pushes, (far_l + 1) * BASE, far_l + 1).astype(F32), 0.0)
    wide = (tiles, lanes)
    lane_w = iota(wide, 1)
    kinds = []
    for kind in range(2):
        here = line_s == lane_w + kind * lanes
        packed = jnp.sum(jnp.where(here, pack_s, 0), axis=0, keepdims=True)
        there = packed > 0
        packed = jnp.where(there, packed - 1, 0)
        local = jnp.clip((packed >> 6) & (BASE - 1), 0, rb - 1)
        kinds.append(jnp.clip(packed >> 12, 0, tiles - 1))
        kinds.append(jnp.where(there, local, BASE) if kind == 0 else local)
        if kind == 0:
            kinds.append(jnp.clip(packed & (BASE - 1), 0, rb - 1))
    for index, value in enumerate(kinds):
        table_v[index : index + 1, :] = value
    table_copy = pltpu.make_async_copy(table_v, table, table_sem)
    table_copy.start()
    code = jnp.sum(jnp.where(name_s == lane_w, code_s, 0.0), axis=0, keepdims=True)
    code = code[:, 0:128]

    wbuf[...] = jnp.zeros(wbuf.shape, F32)
    wbuf[0:rb, :] = -defect_ref[...]
    vector = wbuf[...]
    lane_1 = iota((1, 128), 1)
    code = jnp.where(lane_1 == me * slots, total(vector * vector), code)
    send0[0:rb, 0, :] = -defect_ref[...]
    send0[rb, :, :] = code
    codes[n - 1 : n, :] = code

    pl.semaphore_wait(barrier, n - 1)

    def send(phase, group, source, target, size, spread):
        for place in range(*groups[group]):
            span = pl.ds(place * size, size)
            pltpu.make_async_remote_copy(
                src_ref=source.at[span] if spread else source,
                dst_ref=target.at[span],
                send_sem=sent.at[phase],
                recv_sem=got.at[phase, group],
                device_id=(peer[place],),
                device_id_type=MESH,
            ).start()

    def await_group(phase, group, target, size):
        first, last = groups[group]
        view = target.at[pl.ds(first * size, (last - first) * size)]
        pltpu.make_async_copy(view, view, got.at[phase, group]).wait()

    def await_sent(phase, target, size):
        view = target.at[pl.ds(0, (n - 1) * size)]
        pltpu.make_async_copy(view, view, sent.at[phase]).wait()

    core = me % 2

    def first_copy(source, group, device, spot, size, sem):
        return pltpu.make_async_remote_copy(
            src_ref=source,
            dst_ref=recv0.at[pl.ds(spot * head, size * head)],
            send_sem=sem,
            recv_sem=got.at[0, group],
            device_id=(device,),
            device_id_type=MESH,
        )

    for group in range(count):
        for place in range(groups[group][0], groups[group][1], 2):
            if place < n - 2:
                device, spot = peer[place + 1] + 1 - core, place + core
            else:
                device, spot = peer[place], place
            first_copy(send0, group, device, spot, 1, sent.at[0]).start()

    def pass_on(group):
        first, last = groups[group]
        last = min(last, n - 2)
        part = recv0.at[pl.ds(first * head, (last - first) * head)]
        return first_copy(part, group, peer[n - 2], first, last - first, passed)

    lane_k = iota((width, 128), 1)
    sub = iota((pad, 128), 0)
    sub_f = sub.astype(F32)
    empty = jnp.zeros((width, 128), F32)

    def slots_of(group):
        first, last = groups[group]
        return [(place, slot) for place in range(first, last) for slot in range(slots)]

    def product(tile, row):
        return jnp.sum(tile * row, axis=1, keepdims=True)

    def spread(vector):
        wbuf[...] = vector
        filled = jnp.concatenate([vector, jnp.zeros((width - pad, 128), F32)], axis=0)
        turned = filled.T
        for index in range(rb):
            held[index] = jnp.broadcast_to(turned[:, index : index + 1], (width, 128))

    def push_group(turn, group):
        for place, slot in slots_of(group):
            line = place * slots + slot
            value = far_t[line] * held[table[4, line]]
            send_b[turn, line, :, :] = jnp.sum(value, axis=0, keepdims=True)
        send(1 + 2 * turn, group, send_b.at[turn], recv_b.at[turn], slots, True)

    def own_rows(image):
        for index in range(rb):
            value = jnp.sum(diag_t[index] * held[index], axis=0, keepdims=True)
            image = image + jnp.where(sub == index, value, 0.0)
        return image

    def fetch_all(image, ready, source, between):
        acc = empty
        for group in near_first:
            ready(group)
            for place, slot in slots_of(group):
                line = place * slots + slot
                value = product(coup[table[0, line]], source(place, slot))
                acc = acc + jnp.where(lane_k == table[1, line], value, 0.0)
            image = between(group, image)
        return image + acc.T[0:pad, :]

    def land_group(turn, group, image):
        for place, slot in slots_of(group):
            here = goal_ref[slot, place : place + 1, :] == sub_f
            line = recv_b[turn, place * slots + slot, :, :]
            image = image + jnp.where(here, line, 0.0)
        return image

    def decode(first, last):
        shape = (last - first, 128)
        found = codes[first:last, :]
        lane = iota(shape, 1)
        for slot in range(slots):
            mine = jnp.where(lane == me * slots + slot, found, 0.0)
            value = jnp.sum(mine, axis=1, keepdims=True)
            goal = jnp.floor(value * (1.0 / BASE))
            goal_ref[slot, first:last, :] = jnp.broadcast_to(goal - 1.0, shape)
            ask_ref[slot, first:last, :] = jnp.broadcast_to(value - goal * BASE - 1.0, shape)

    def gather_group(turn, group, vector):
        for place, slot in slots_of(group):
            here = ask_ref[slot, place : place + 1, :] == sub_f
            line = jnp.sum(jnp.where(here, vector, 0.0), axis=0, keepdims=True)
            send_a[turn - 1, place * lines + slot, :, :] = line

    def send_asked(turn, group, own_part):
        for place in range(*groups[group]):
            send_a[turn - 1, place * lines + slots, :, :] = own_part
        send(2 * turn, group, send_a.at[turn - 1], recv_a.at[turn - 1], lines, True)

    for item in loads:
        item.wait()
    table_copy.wait()
    mass = jnp.concatenate([mass_ref[...], jnp.zeros((pad - rb, 128), F32)], axis=0)

    urgent = list(range(min(3, count)))
    cut = min(-(-groups[min(1, count - 1)][1] // 8) * 8, n)
    early = [group for group in reversed(range(count)) if groups[group][0] >= cut]
    near_first = list(reversed(range(count)))
    spread(vector)
    for group in range(count):
        for place, slot in slots_of(group):
            line = place * slots + slot
            far_t[line] = coup[table[3, line]].T
        push_group(0, group)
    for index in range(rb):
        diag_t[index] = diag[index].T
    image = own_rows(mass * vector)
    landed = {2: near_first[:2], 1: near_first[2:-2]} if count > 3 else {1: near_first[:-2]}

    def ready_first(group):
        await_group(0, group, recv0, head)
        pl.when(core == 1)(pass_on(group).start)
        for place in range(*groups[group]):
            spot = place
            if place < n - 2:
                spot = place + (1 - core) * (1 - 2 * (place % 2))
            codes[place : place + 1, :] = recv0[spot * head + rb]
            for row in range(rb):
                blocks[place * rb + row, :, :] = recv0[spot * head + row]

    def block_row(place, slot):
        return blocks[place * rb + table[2, place * slots + slot]]

    def between_first(group, image):
        if group == 1:
            if cut < n:
                decode(cut, n)
            for other in early:
                await_group(1, other, recv_b.at[0], slots)
                image = land_group(0, other, image)
        return image

    image = fetch_all(image, ready_first, block_row, between_first)
    decode(0, cut)
    places = iota((n, 1), 0)
    whose = sum(jnp.where(places == at, mask, 0) for at, mask in enumerate(masks)) ^ me
    squares = total(jnp.where(iota((n, 128), 1) == whose * slots, codes[...], 0.0))
    beta = jnp.sqrt(squares)
    for group in near_first:
        if group in early:
            continue
        await_group(1, group, recv_b.at[0], slots)
        image = land_group(0, group, image)
    basis = [vector / beta]
    images = [image / beta]
    heads = []
    gram = {}

    for turn in range(1, ITERS):
        vector = images[-1]
        own_part = as_row(
            [total(vector * item) for item in basis]
            + [total(vector * item) for item in images]
        )
        for group in urgent:
            gather_group(turn, group, vector)
            send_asked(turn, group, own_part)
        spread(vector)
        for group in urgent[:2]:
            push_group(turn, group)
        for group in range(len(urgent), count):
            gather_group(turn, group, vector)
            send_asked(turn, group, own_part)
        for group in range(len(urgent[:2]), count):
            push_group(turn, group)
        image = own_rows(mass * vector)
        parts_of = [own_part]

        def ready(group):
            await_group(2 * turn, group, recv_a.at[turn - 1], lines)
            for place in range(*groups[group]):
                parts_of.append(recv_a[turn - 1, place * lines + slots, :, :])

        def asked_row(place, slot):
            return recv_a[turn - 1, place * lines + slot, :, :]

        def between(group, image):
            for other in landed.get(group, ()):
                await_group(1 + 2 * turn, other, recv_b.at[turn], slots)
                image = land_group(turn, other, image)
            return image

        image = fetch_all(image, ready, asked_row, between)
        sums = sum(parts_of[1:], parts_of[0])
        dots = [pick(sums, index) for index in range(turn)]
        for index in range(turn):
            gram[index, turn - 1] = pick(sums, turn + index)
        heads.append(dots[0])
        square = gram[turn - 1, turn - 1]
        left = square
        for value in dots:
            left = left - value * value
        scale = lax.rsqrt(jnp.maximum(left, square * 1e-6))
        for index in range(turn):
            vector = vector - dots[index] * basis[index]
        basis.append(vector * scale)
        for group in near_first[-2:]:
            await_group(1 + 2 * turn, group, recv_b.at[turn], slots)
            image = land_group(turn, group, image)
        for index in range(turn):
            image = image - dots[index] * images[index]
        images.append(image * scale)

    vector = images[-1]
    own_part = as_row(
        [total(vector * basis[0])] + [total(vector * item) for item in images]
    )
    send_f[0] = own_part
    last_phase = 2 * ITERS
    for group in range(count):
        send(last_phase, group, send_f, recv_f, 1, False)
    sums = own_part
    for group in near_first:
        await_group(last_phase, group, recv_f, 1)
        for place in range(*groups[group]):
            sums = sums + recv_f[place, :, :]
    heads.append(pick(sums, 0))
    for index in range(ITERS):
        gram[index, ITERS - 1] = pick(sums, 1 + index)

    factor = {}
    for i in range(ITERS):
        for j in range(i + 1):
            value = gram[j, i]
            for k in range(j):
                value = value - factor[i, k] * factor[j, k]
            factor[i, j] = jnp.sqrt(value) if i == j else value / factor[j, j]
    forward = []
    for i in range(ITERS):
        value = beta * heads[i]
        for k in range(i):
            value = value - factor[i, k] * forward[k]
        forward.append(value / factor[i, i])
    mixing = [None] * ITERS
    for i in reversed(range(ITERS)):
        value = forward[i]
        for k in range(i + 1, ITERS):
            value = value - factor[k, i] * mixing[k]
        mixing[i] = value / factor[i, i]
    update = mixing[0] * basis[0]
    for i in range(1, ITERS):
        update = update + mixing[i] * basis[i]
    out_ref[...] = update[0:rb, :]

    view = recv0.at[pl.ds(0, n // 2 * head)]
    pltpu.make_async_copy(view, view, sent.at[0]).wait()
    whole = recv0.at[pl.ds(0, (n - 2) * head)]
    pl.when(core == 1)(pltpu.make_async_copy(whole, whole, passed).wait)
    for turn in range(ITERS):
        await_sent(1 + 2 * turn, recv_b.at[turn], slots)
    for turn in range(1, ITERS):
        await_sent(2 * turn, recv_a.at[turn - 1], lines)
    await_sent(last_phase, recv_f, 1)


def on_device(defect, mass, block_diag, coupling, tile_rows, tile_cols):
    rb, width = defect.shape
    tiles = tile_rows.shape[0]
    n = lax.axis_size("blk")
    slots = (tiles // 2 + n - 2) // (n - 1)
    lines = slots + 1
    pad = -(-rb // 8) * 8
    lanes = -(-n * slots // 128) * 128
    hbm = pl.BlockSpec(memory_space=pltpu.HBM)
    phases = 2 * ITERS + 1
    return pl.pallas_call(
        functools.partial(kernel, n, slots),
        out_shape=pltpu.VMEM((rb, width), F32),
        in_specs=[hbm] * 6,
        out_specs=pl.BlockSpec(memory_space=pltpu.VMEM),
        scratch_shapes=[
            pltpu.VMEM((tiles, width, width), F32),
            pltpu.VMEM((rb, width, width), F32),
            pltpu.VMEM((rb, width), F32),
            pltpu.VMEM((rb, width), F32),
            pltpu.VMEM((1, tiles), I32),
            pltpu.VMEM((1, tiles), I32),
            pltpu.VMEM((8, lanes), I32),
            pltpu.SMEM((8, lanes), I32),
            pltpu.VMEM((pad, width), F32),
            pltpu.VMEM((rb, width, width), F32),
            pltpu.VMEM(((n - 1) * slots, width, width), F32),
            pltpu.VMEM((rb, width, width), F32),
            pltpu.VMEM((n, width), F32),
            pltpu.VMEM((slots, n, width), F32),
            pltpu.VMEM((slots, n, width), F32),
            pltpu.VMEM((rb + 1, 1, width), F32),
            pltpu.VMEM((n * (rb + 1), 1, width), F32),
            pltpu.VMEM((n * rb, 1, width), F32),
            pltpu.VMEM((ITERS - 1, n * lines, 1, width), F32),
            pltpu.VMEM((ITERS - 1, n * lines, 1, width), F32),
            pltpu.VMEM((ITERS, n * slots, 1, width), F32),
            pltpu.VMEM((ITERS, n * slots, 1, width), F32),
            pltpu.VMEM((1, 1, width), F32),
            pltpu.VMEM((n, 1, width), F32),
            pltpu.SemaphoreType.DMA((9,)),
            pltpu.SemaphoreType.DMA,
            pltpu.SemaphoreType.DMA((phases,)),
            pltpu.SemaphoreType.DMA,
            pltpu.SemaphoreType.DMA((phases, len(layout(n)[1]))),
        ],
        compiler_params=pltpu.CompilerParams(
            collective_id=0, has_side_effects=True, vmem_limit_bytes=VMEM_LIMIT
        ),
    )(
        defect,
        mass,
        block_diag,
        coupling,
        tile_rows.reshape(1, tiles),
        tile_cols.reshape(1, tiles),
    )


def solution(mesh):
    in_specs = (
        P("blk", None),
        P("blk", None),
        P("blk", None, None),
        P("blk", None, None),
        P("blk"),
        P("blk"),
    )
    return jax.shard_map(
        on_device, mesh=mesh, in_specs=in_specs, out_specs=P("blk", None), check_vma=False
    )
```

```python
import functools

import jax
import jax.numpy as jnp
from jax import lax
from jax.experimental import pallas as pl
from jax.experimental.pallas import tpu as pltpu
from jax.sharding import PartitionSpec as P

ITERS = 3
F32 = jnp.float32
I32 = jnp.int32
MESH = pl.DeviceIdType.MESH
BASE = 64
VMEM_LIMIT = 57 * 1024 * 1024


def iota(shape, axis):
    return lax.broadcasted_iota(I32, shape, axis)


def iota_f(shape, axis):
    return iota(shape, axis).astype(F32)


def total(value):
    return jnp.sum(jnp.sum(value, axis=0, keepdims=True), axis=1, keepdims=True)


def as_row(items):
    lane = iota((1, 128), 1)
    row = jnp.zeros((1, 128), F32)
    for index, item in enumerate(items):
        row = jnp.where(lane == index, item, row)
    return row


def pick(row, index):
    lane = iota((1, 128), 1)
    return jnp.sum(jnp.where(lane == index, row, 0.0), axis=1, keepdims=True)


def layout(n):
    def far(chip):
        return min((chip & 1) + (chip >> 1 & 1) + (chip >> 2), 5)

    chips = sorted(range(n // 2), key=lambda chip: (-far(chip), -chip))
    masks = [2 * chip + bit for chip in chips for bit in (1, 0)]
    levels = [max(far(mask // 2), 1) for mask in masks[: n - 1]]
    starts = [at for at in range(n - 1) if at == 0 or levels[at] != levels[at - 1]]
    return masks, list(zip(starts, starts[1:] + [n - 1]))


def kernel(
    n,
    slots,
    defect_hbm,
    mass_hbm,
    diag_hbm,
    coup_hbm,
    rows_hbm,
    cols_hbm,
    out_ref,
    coup,
    diag,
    defect_ref,
    mass_ref,
    rows_ref,
    cols_ref,
    table_v,
    table,
    wbuf,
    held,
    far_t,
    diag_t,
    codes,
    ask_ref,
    goal_ref,
    send0,
    recv0,
    blocks,
    send_a,
    recv_a,
    send_b,
    recv_b,
    send_f,
    recv_f,
    load_sems,
    table_sem,
    sent,
    passed,
    got,
):
    me = lax.axis_index("blk")
    rb, width = defect_ref.shape
    tiles = rows_ref.shape[1]
    pad = wbuf.shape[0]
    lanes = table.shape[1]
    parts = 4
    chunk = tiles // parts
    masks, groups = layout(n)
    count = len(groups)
    head = rb + 1
    lines = slots + 1

    peers = {0: me}
    for mask in range(1, n):
        low_bit = mask & -mask
        sign = 1 - 2 * ((me // low_bit) % 2)
        peers[mask] = peers[mask - low_bit] + sign * low_bit
    peer = [peers[mask] for mask in masks]

    small = [
        pltpu.make_async_copy(rows_hbm, rows_ref, load_sems.at[parts + 1]),
        pltpu.make_async_copy(cols_hbm, cols_ref, load_sems.at[parts + 2]),
        pltpu.make_async_copy(defect_hbm, defect_ref, load_sems.at[parts + 3]),
        pltpu.make_async_copy(mass_hbm, mass_ref, load_sems.at[parts + 4]),
    ]
    for item in small:
        item.start()

    barrier = pltpu.get_barrier_semaphore()
    for place in range(n - 1):
        pl.semaphore_signal(barrier, inc=1, device_id=(peer[place],), device_id_type=MESH)

    loads = []
    for part in range(parts):
        span = pl.ds(part * chunk, chunk)
        loads.append(
            pltpu.make_async_copy(coup_hbm.at[span], coup.at[span], load_sems.at[part])
        )
    loads.append(pltpu.make_async_copy(diag_hbm, diag, load_sems.at[parts]))
    for item in loads:
        item.start()
    for item in small:
        item.wait()

    rows = rows_ref[...]
    cols = cols_ref[...]
    low = me * rb
    pushes = (rows < low) | (rows >= low + rb)
    push_l = jnp.where(pushes, 1, 0)
    rem_l = jnp.where(pushes, rows, cols)
    loc_l = jnp.where(pushes, cols, rows) - low
    own_l = (rem_l * (-(-65536 // rb))) >> 16
    far_l = rem_l - own_l * rb
    square = (tiles, tiles)
    eye = iota(square, 0) == iota(square, 1)
    earlier = iota(square, 0) < iota(square, 1)

    def to_s(value, zero):
        return jnp.sum(jnp.where(eye, value, zero), axis=1, keepdims=True)

    key_l = own_l + push_l * n
    key_s = to_s(key_l, 0)
    slot_l = jnp.sum(jnp.where((key_s == key_l) & earlier, 1, 0), axis=0, keepdims=True)
    apart = own_l ^ me
    place_l = sum(jnp.where(apart == mask, at, 0) for at, mask in enumerate(masks))
    line_l = place_l * slots + slot_l
    tile_l = iota((1, tiles), 1)
    line_s = to_s(line_l + push_l * lanes, 0)
    pack_s = to_s(((tile_l * BASE + loc_l) * BASE + far_l) + 1, 0)
    name_s = to_s(own_l * slots + slot_l, 0)
    code_s = to_s(jnp.where(pushes, (far_l + 1) * BASE, far_l + 1).astype(F32), 0.0)
    wide = (tiles, lanes)
    lane_w = iota(wide, 1)
    kinds = []
    for kind in range(2):
        here = line_s == lane_w + kind * lanes
        packed = jnp.sum(jnp.where(here, pack_s, 0), axis=0, keepdims=True)
        there = packed > 0
        packed = jnp.where(there, packed - 1, 0)
        local = jnp.clip((packed >> 6) & (BASE - 1), 0, rb - 1)
        kinds.append(jnp.clip(packed >> 12, 0, tiles - 1))
        kinds.append(jnp.where(there, local, BASE) if kind == 0 else local)
        if kind == 0:
            kinds.append(jnp.clip(packed & (BASE - 1), 0, rb - 1))
    for index, value in enumerate(kinds):
        table_v[index : index + 1, :] = value
    table_copy = pltpu.make_async_copy(table_v, table, table_sem)
    table_copy.start()
    code = jnp.sum(jnp.where(name_s == lane_w, code_s, 0.0), axis=0, keepdims=True)
    code = code[:, 0:128]

    wbuf[...] = jnp.zeros(wbuf.shape, F32)
    wbuf[0:rb, :] = -defect_ref[...]
    vector = wbuf[...]
    lane_1 = iota((1, 128), 1)
    code = jnp.where(lane_1 == me * slots, total(vector * vector), code)
    send0[0:rb, 0, :] = -defect_ref[...]
    send0[rb, :, :] = code
    codes[n - 1 : n, :] = code

    pl.semaphore_wait(barrier, n - 1)

    def send(phase, group, source, target, size, spread):
        for place in range(*groups[group]):
            span = pl.ds(place * size, size)
            pltpu.make_async_remote_copy(
                src_ref=source.at[span] if spread else source,
                dst_ref=target.at[span],
                send_sem=sent.at[phase],
                recv_sem=got.at[phase, group],
                device_id=(peer[place],),
                device_id_type=MESH,
            ).start()

    def await_group(phase, group, target, size):
        first, last = groups[group]
        view = target.at[pl.ds(first * size, (last - first) * size)]
        pltpu.make_async_copy(view, view, got.at[phase, group]).wait()

    def await_sent(phase, target, size):
        view = target.at[pl.ds(0, (n - 1) * size)]
        pltpu.make_async_copy(view, view, sent.at[phase]).wait()

    core = me % 2

    def first_copy(source, group, device, spot, size, sem):
        return pltpu.make_async_remote_copy(
            src_ref=source,
            dst_ref=recv0.at[pl.ds(spot * head, size * head)],
            send_sem=sem,
            recv_sem=got.at[0, group],
            device_id=(device,),
            device_id_type=MESH,
        )

    for group in range(count):
        for place in range(groups[group][0], groups[group][1], 2):
            if place < n - 2:
                device, spot = peer[place + 1] + 1 - core, place + core
            else:
                device, spot = peer[place], place
            first_copy(send0, group, device, spot, 1, sent.at[0]).start()

    def pass_on(group):
        first, last = groups[group]
        last = min(last, n - 2)
        part = recv0.at[pl.ds(first * head, (last - first) * head)]
        return first_copy(part, group, peer[n - 2], first, last - first, passed)

    lane_k = iota((width, 128), 1)
    sub = iota((pad, 128), 0)
    sub_f = sub.astype(F32)
    empty = jnp.zeros((width, 128), F32)

    def slots_of(group):
        first, last = groups[group]
        return [(place, slot) for place in range(first, last) for slot in range(slots)]

    def product(tile, row):
        return jnp.sum(tile * row, axis=1, keepdims=True)

    def turn_over(vector):
        filled = jnp.concatenate([vector, jnp.zeros((width - pad, 128), F32)], axis=0)
        return filled.T

    def spread(turned):
        for index in range(rb):
            held[index] = jnp.broadcast_to(turned[:, index : index + 1], (width, 128))

    def push_group(turn, group):
        for place, slot in slots_of(group):
            line = place * slots + slot
            value = far_t[line] * held[table[4, line]]
            send_b[turn, line, :, :] = jnp.sum(value, axis=0, keepdims=True)
        send(1 + 2 * turn, group, send_b.at[turn], recv_b.at[turn], slots, True)

    ones = jnp.ones((2 * width, 128), jnp.bfloat16)

    def product_too(tile, row):
        value = tile * row
        high = value.astype(jnp.bfloat16)
        rest = (value - high.astype(F32)).astype(jnp.bfloat16)
        return jnp.dot(
            jnp.concatenate([high, rest], axis=1), ones, preferred_element_type=F32
        )

    def own_rows(image):
        for index in range(rb):
            value = jnp.sum(diag_t[index] * held[index], axis=0, keepdims=True)
            image = image + jnp.where(sub == index, value, 0.0)
        return image

    def fetch_all(image, ready, source, between):
        acc = empty
        for group in near_first:
            ready(group)
            for index, (place, slot) in enumerate(slots_of(group)):
                line = place * slots + slot
                by = product_too if group > 0 and index % 3 == 1 else product
                value = by(coup[table[0, line]], source(place, slot))
                acc = acc + jnp.where(lane_k == table[1, line], value, 0.0)
            image = between(group, image)
        return image + acc.T[0:pad, :]

    def land_group(turn, group, image):
        for place, slot in slots_of(group):
            here = goal_ref[slot, place : place + 1, :] == sub_f
            line = recv_b[turn, place * slots + slot, :, :]
            image = image + jnp.where(here, line, 0.0)
        return image

    def decode(first, last):
        shape = (last - first, 128)
        found = codes[first:last, :]
        lane = iota(shape, 1)
        for slot in range(slots):
            mine = jnp.where(lane == me * slots + slot, found, 0.0)
            value = jnp.sum(mine, axis=1, keepdims=True)
            goal = jnp.floor(value * (1.0 / BASE))
            goal_ref[slot, first:last, :] = jnp.broadcast_to(goal - 1.0, shape)
            ask_ref[slot, first:last, :] = jnp.broadcast_to(value - goal * BASE - 1.0, shape)

    def gather_group(turn, group, vector):
        for place, slot in slots_of(group):
            here = ask_ref[slot, place : place + 1, :] == sub_f
            line = jnp.sum(jnp.where(here, vector, 0.0), axis=0, keepdims=True)
            send_a[turn - 1, place * lines + slot, :, :] = line

    def send_asked(turn, group, own_part):
        for place in range(*groups[group]):
            send_a[turn - 1, place * lines + slots, :, :] = own_part
        send(2 * turn, group, send_a.at[turn - 1], recv_a.at[turn - 1], lines, True)

    for item in loads:
        item.wait()
    table_copy.wait()
    mass = jnp.concatenate([mass_ref[...], jnp.zeros((pad - rb, 128), F32)], axis=0)

    urgent = list(range(count))
    cut = min(-(-groups[min(1, count - 1)][1] // 8) * 8, n)
    early = [group for group in reversed(range(count)) if groups[group][0] >= cut]
    near_first = list(reversed(range(count)))
    spread(turn_over(vector))
    for group in range(count):
        for place, slot in slots_of(group):
            line = place * slots + slot
            far_t[line] = coup[table[3, line]].T
        push_group(0, group)
    for index in range(rb):
        diag_t[index] = diag[index].T
    image = own_rows(mass * vector)
    landed = {2: near_first[:2], 1: near_first[2:-2]} if count > 3 else {1: near_first[:-2]}

    def ready_first(group):
        await_group(0, group, recv0, head)
        pl.when(core == 1)(pass_on(group).start)
        for place in range(*groups[group]):
            spot = place
            if place < n - 2:
                spot = place + (1 - core) * (1 - 2 * (place % 2))
            codes[place : place + 1, :] = recv0[spot * head + rb]
            for row in range(rb):
                blocks[place * rb + row, :, :] = recv0[spot * head + row]

    def block_row(place, slot):
        return blocks[place * rb + table[2, place * slots + slot]]

    def between_first(group, image):
        if group == 1:
            if cut < n:
                decode(cut, n)
            for other in early:
                await_group(1, other, recv_b.at[0], slots)
                image = land_group(0, other, image)
        return image

    image = fetch_all(image, ready_first, block_row, between_first)
    decode(0, cut)
    places = iota((n, 1), 0)
    whose = sum(jnp.where(places == at, mask, 0) for at, mask in enumerate(masks)) ^ me
    squares = total(jnp.where(iota((n, 128), 1) == whose * slots, codes[...], 0.0))
    beta = jnp.sqrt(squares)
    for group in near_first:
        if group in early:
            continue
        await_group(1, group, recv_b.at[0], slots)
        image = land_group(0, group, image)
    basis = [vector / beta]
    images = [image / beta]
    heads = []
    gram = {}

    for turn in range(1, ITERS):
        vector = images[-1]
        own_part = as_row(
            [total(vector * item) for item in basis]
            + [total(vector * item) for item in images]
        )
        turned = turn_over(vector)
        for group in urgent:
            gather_group(turn, group, vector)
            send_asked(turn, group, own_part)
        spread(turned)
        for group in urgent[:2]:
            push_group(turn, group)
        for group in range(len(urgent), count):
            gather_group(turn, group, vector)
            send_asked(turn, group, own_part)
        for group in range(len(urgent[:2]), count):
            push_group(turn, group)
        image = own_rows(mass * vector)
        parts_of = [own_part]

        def ready(group):
            await_group(2 * turn, group, recv_a.at[turn - 1], lines)
            for place in range(*groups[group]):
                parts_of.append(recv_a[turn - 1, place * lines + slots, :, :])

        def asked_row(place, slot):
            return recv_a[turn - 1, place * lines + slot, :, :]

        def between(group, image):
            for other in landed.get(group, ()):
                await_group(1 + 2 * turn, other, recv_b.at[turn], slots)
                image = land_group(turn, other, image)
            return image

        image = fetch_all(image, ready, asked_row, between)
        sums = sum(parts_of[1:], parts_of[0])
        dots = [pick(sums, index) for index in range(turn)]
        for index in range(turn):
            gram[index, turn - 1] = pick(sums, turn + index)
        heads.append(dots[0])
        square = gram[turn - 1, turn - 1]
        left = square
        for value in dots:
            left = left - value * value
        scale = lax.rsqrt(jnp.maximum(left, square * 1e-6))
        for index in range(turn):
            vector = vector - dots[index] * basis[index]
        basis.append(vector * scale)
        for group in near_first[-2:]:
            await_group(1 + 2 * turn, group, recv_b.at[turn], slots)
            image = land_group(turn, group, image)
        for index in range(turn):
            image = image - dots[index] * images[index]
        images.append(image * scale)

    vector = images[-1]
    own_part = as_row(
        [total(vector * basis[0])] + [total(vector * item) for item in images]
    )
    send_f[0] = own_part
    last_phase = 2 * ITERS
    for group in range(count):
        send(last_phase, group, send_f, recv_f, 1, False)
    view = recv0.at[pl.ds(0, n // 2 * head)]
    pltpu.make_async_copy(view, view, sent.at[0]).wait()
    whole = recv0.at[pl.ds(0, (n - 2) * head)]
    pl.when(core == 1)(pltpu.make_async_copy(whole, whole, passed).wait)
    for turn in range(ITERS):
        await_sent(1 + 2 * turn, recv_b.at[turn], slots)
    for turn in range(1, ITERS):
        await_sent(2 * turn, recv_a.at[turn - 1], lines)
    factor = {}
    forward = []

    def eliminate(i):
        for j in range(i + 1):
            value = gram[j, i]
            for k in range(j):
                value = value - factor[i, k] * factor[j, k]
            factor[i, j] = jnp.sqrt(value) if i == j else value / factor[j, j]
        value = beta * heads[i]
        for k in range(i):
            value = value - factor[i, k] * forward[k]
        forward.append(value / factor[i, i])

    for i in range(ITERS - 1):
        eliminate(i)
    sums = own_part
    for group in near_first:
        await_group(last_phase, group, recv_f, 1)
        for place in range(*groups[group]):
            sums = sums + recv_f[place, :, :]
    heads.append(pick(sums, 0))
    for index in range(ITERS):
        gram[index, ITERS - 1] = pick(sums, 1 + index)

    eliminate(ITERS - 1)
    mixing = [None] * ITERS
    for i in reversed(range(ITERS)):
        value = forward[i]
        for k in range(i + 1, ITERS):
            value = value - factor[k, i] * mixing[k]
        mixing[i] = value / factor[i, i]
    update = mixing[0] * basis[0]
    for i in range(1, ITERS):
        update = update + mixing[i] * basis[i]
    out_ref[...] = update[0:rb, :]

    await_sent(last_phase, recv_f, 1)


def on_device(defect, mass, block_diag, coupling, tile_rows, tile_cols):
    rb, width = defect.shape
    tiles = tile_rows.shape[0]
    n = lax.axis_size("blk")
    slots = (tiles // 2 + n - 2) // (n - 1)
    lines = slots + 1
    pad = -(-rb // 8) * 8
    lanes = -(-n * slots // 128) * 128
    hbm = pl.BlockSpec(memory_space=pltpu.HBM)
    phases = 2 * ITERS + 1
    return pl.pallas_call(
        functools.partial(kernel, n, slots),
        out_shape=pltpu.VMEM((rb, width), F32),
        in_specs=[hbm] * 6,
        out_specs=pl.BlockSpec(memory_space=pltpu.VMEM),
        scratch_shapes=[
            pltpu.VMEM((tiles, width, width), F32),
            pltpu.VMEM((rb, width, width), F32),
            pltpu.VMEM((rb, width), F32),
            pltpu.VMEM((rb, width), F32),
            pltpu.VMEM((1, tiles), I32),
            pltpu.VMEM((1, tiles), I32),
            pltpu.VMEM((8, lanes), I32),
            pltpu.SMEM((8, lanes), I32),
            pltpu.VMEM((pad, width), F32),
            pltpu.VMEM((rb, width, width), F32),
            pltpu.VMEM(((n - 1) * slots, width, width), F32),
            pltpu.VMEM((rb, width, width), F32),
            pltpu.VMEM((n, width), F32),
            pltpu.VMEM((slots, n, width), F32),
            pltpu.VMEM((slots, n, width), F32),
            pltpu.VMEM((rb + 1, 1, width), F32),
            pltpu.VMEM((n * (rb + 1), 1, width), F32),
            pltpu.VMEM((n * rb, 1, width), F32),
            pltpu.VMEM((ITERS - 1, n * lines, 1, width), F32),
            pltpu.VMEM((ITERS - 1, n * lines, 1, width), F32),
            pltpu.VMEM((ITERS, n * slots, 1, width), F32),
            pltpu.VMEM((ITERS, n * slots, 1, width), F32),
            pltpu.VMEM((1, 1, width), F32),
            pltpu.VMEM((n, 1, width), F32),
            pltpu.SemaphoreType.DMA((9,)),
            pltpu.SemaphoreType.DMA,
            pltpu.SemaphoreType.DMA((phases,)),
            pltpu.SemaphoreType.DMA,
            pltpu.SemaphoreType.DMA((phases, len(layout(n)[1]))),
        ],
        compiler_params=pltpu.CompilerParams(
            collective_id=0, has_side_effects=True, vmem_limit_bytes=VMEM_LIMIT
        ),
    )(
        defect,
        mass,
        block_diag,
        coupling,
        tile_rows.reshape(1, tiles),
        tile_cols.reshape(1, tiles),
    )


def solution(mesh):
    in_specs = (
        P("blk", None),
        P("blk", None),
        P("blk", None, None),
        P("blk", None, None),
        P("blk"),
        P("blk"),
    )
    return jax.shard_map(
        on_device, mesh=mesh, in_specs=in_specs, out_specs=P("blk", None), check_vma=False
    )
```

```python
import functools

import jax
import jax.numpy as jnp
from jax import lax
from jax.experimental import pallas as pl
from jax.experimental.pallas import tpu as pltpu
from jax.sharding import PartitionSpec as P

ITERS = 3
F32 = jnp.float32
I32 = jnp.int32
MESH = pl.DeviceIdType.MESH
BASE = 64
VMEM_LIMIT = 57 * 1024 * 1024


def iota(shape, axis):
    return lax.broadcasted_iota(I32, shape, axis)


def iota_f(shape, axis):
    return iota(shape, axis).astype(F32)


def total(value):
    return jnp.sum(jnp.sum(value, axis=0, keepdims=True), axis=1, keepdims=True)


def as_row(items):
    lane = iota((1, 128), 1)
    row = jnp.zeros((1, 128), F32)
    for index, item in enumerate(items):
        row = jnp.where(lane == index, item, row)
    return row


def pick(row, index):
    lane = iota((1, 128), 1)
    return jnp.sum(jnp.where(lane == index, row, 0.0), axis=1, keepdims=True)


def layout(n):
    def far(chip):
        return min((chip & 1) + (chip >> 1 & 1) + (chip >> 2), 5)

    chips = sorted(range(n // 2), key=lambda chip: (-far(chip), -chip))
    masks = [2 * chip + bit for chip in chips for bit in (1, 0)]
    levels = [max(far(mask // 2), 1) for mask in masks[: n - 1]]
    starts = [at for at in range(n - 1) if at == 0 or levels[at] != levels[at - 1]]
    return masks, list(zip(starts, starts[1:] + [n - 1]))


def kernel(
    n,
    slots,
    defect_hbm,
    mass_hbm,
    diag_hbm,
    coup_hbm,
    rows_hbm,
    cols_hbm,
    out_ref,
    coup,
    diag,
    defect_ref,
    mass_ref,
    rows_ref,
    cols_ref,
    table_v,
    table,
    wbuf,
    held,
    far_t,
    diag_t,
    codes,
    ask_ref,
    goal_ref,
    send0,
    recv0,
    blocks,
    send_a,
    recv_a,
    send_b,
    recv_b,
    send_f,
    recv_f,
    load_sems,
    table_sem,
    sent,
    passed,
    got,
):
    me = lax.axis_index("blk")
    rb, width = defect_ref.shape
    tiles = rows_ref.shape[1]
    pad = wbuf.shape[0]
    lanes = table.shape[1]
    parts = 4
    chunk = tiles // parts
    masks, groups = layout(n)
    count = len(groups)
    head = rb + 1
    lines = slots + 1

    peers = {0: me}
    for mask in range(1, n):
        low_bit = mask & -mask
        sign = 1 - 2 * ((me // low_bit) % 2)
        peers[mask] = peers[mask - low_bit] + sign * low_bit
    peer = [peers[mask] for mask in masks]

    small = [
        pltpu.make_async_copy(rows_hbm, rows_ref, load_sems.at[parts + 1]),
        pltpu.make_async_copy(cols_hbm, cols_ref, load_sems.at[parts + 2]),
        pltpu.make_async_copy(defect_hbm, defect_ref, load_sems.at[parts + 3]),
        pltpu.make_async_copy(mass_hbm, mass_ref, load_sems.at[parts + 4]),
    ]
    for item in small:
        item.start()

    barrier = pltpu.get_barrier_semaphore()
    for place in range(n - 1):
        pl.semaphore_signal(barrier, inc=1, device_id=(peer[place],), device_id_type=MESH)

    loads = []
    for part in range(parts):
        span = pl.ds(part * chunk, chunk)
        loads.append(
            pltpu.make_async_copy(coup_hbm.at[span], coup.at[span], load_sems.at[part])
        )
    loads.append(pltpu.make_async_copy(diag_hbm, diag, load_sems.at[parts]))
    for item in loads:
        item.start()
    for item in small:
        item.wait()

    rows = rows_ref[...]
    cols = cols_ref[...]
    low = me * rb
    pushes = (rows < low) | (rows >= low + rb)
    push_l = jnp.where(pushes, 1, 0)
    rem_l = jnp.where(pushes, rows, cols)
    loc_l = jnp.where(pushes, cols, rows) - low
    own_l = (rem_l * (-(-65536 // rb))) >> 16
    far_l = rem_l - own_l * rb
    square = (tiles, tiles)
    eye = iota(square, 0) == iota(square, 1)
    earlier = iota(square, 0) < iota(square, 1)

    def to_s(value, zero):
        return jnp.sum(jnp.where(eye, value, zero), axis=1, keepdims=True)

    key_l = own_l + push_l * n
    key_s = to_s(key_l, 0)
    slot_l = jnp.sum(jnp.where((key_s == key_l) & earlier, 1, 0), axis=0, keepdims=True)
    apart = own_l ^ me
    place_l = sum(jnp.where(apart == mask, at, 0) for at, mask in enumerate(masks))
    line_l = place_l * slots + slot_l
    tile_l = iota((1, tiles), 1)
    line_s = to_s(line_l + push_l * lanes, 0)
    pack_s = to_s(((tile_l * BASE + loc_l) * BASE + far_l) + 1, 0)
    name_s = to_s(own_l * slots + slot_l, 0)
    code_s = to_s(jnp.where(pushes, (far_l + 1) * BASE, far_l + 1).astype(F32), 0.0)
    wide = (tiles, lanes)
    lane_w = iota(wide, 1)
    kinds = []
    for kind in range(2):
        here = line_s == lane_w + kind * lanes
        packed = jnp.sum(jnp.where(here, pack_s, 0), axis=0, keepdims=True)
        there = packed > 0
        packed = jnp.where(there, packed - 1, 0)
        local = jnp.clip((packed >> 6) & (BASE - 1), 0, rb - 1)
        kinds.append(jnp.clip(packed >> 12, 0, tiles - 1))
        kinds.append(jnp.where(there, local, BASE) if kind == 0 else local)
        if kind == 0:
            kinds.append(jnp.clip(packed & (BASE - 1), 0, rb - 1))
    for index, value in enumerate(kinds):
        table_v[index : index + 1, :] = value
    table_copy = pltpu.make_async_copy(table_v, table, table_sem)
    table_copy.start()
    code = jnp.sum(jnp.where(name_s == lane_w, code_s, 0.0), axis=0, keepdims=True)
    code = code[:, 0:128]

    wbuf[...] = jnp.zeros(wbuf.shape, F32)
    wbuf[0:rb, :] = -defect_ref[...]
    vector = wbuf[...]
    lane_1 = iota((1, 128), 1)
    code = jnp.where(lane_1 == me * slots, total(vector * vector), code)
    send0[0:rb, 0, :] = -defect_ref[...]
    send0[rb, :, :] = code
    codes[n - 1 : n, :] = code

    pl.semaphore_wait(barrier, n - 1)

    def send(phase, group, source, target, size, spread):
        for place in range(*groups[group]):
            span = pl.ds(place * size, size)
            pltpu.make_async_remote_copy(
                src_ref=source.at[span] if spread else source,
                dst_ref=target.at[span],
                send_sem=sent.at[phase],
                recv_sem=got.at[phase, group],
                device_id=(peer[place],),
                device_id_type=MESH,
            ).start()

    def await_group(phase, group, target, size):
        first, last = groups[group]
        view = target.at[pl.ds(first * size, (last - first) * size)]
        pltpu.make_async_copy(view, view, got.at[phase, group]).wait()

    def await_sent(phase, target, size):
        view = target.at[pl.ds(0, (n - 1) * size)]
        pltpu.make_async_copy(view, view, sent.at[phase]).wait()

    core = me % 2

    def first_copy(source, group, device, spot, size, sem):
        return pltpu.make_async_remote_copy(
            src_ref=source,
            dst_ref=recv0.at[pl.ds(spot * head, size * head)],
            send_sem=sem,
            recv_sem=got.at[0, group],
            device_id=(device,),
            device_id_type=MESH,
        )

    plain = [count - 1]
    for group in range(count):
        if group in plain:
            for place in range(*groups[group]):
                first_copy(send0, group, peer[place], place, 1, sent.at[0]).start()
            continue
        for place in range(groups[group][0], groups[group][1], 2):
            if place < n - 2:
                device, spot = peer[place + 1] + 1 - core, place + core
            else:
                device, spot = peer[place], place
            first_copy(send0, group, device, spot, 1, sent.at[0]).start()

    def pass_on(group):
        first, last = groups[group]
        last = min(last, n - 2)
        part = recv0.at[pl.ds(first * head, (last - first) * head)]
        return first_copy(part, group, peer[n - 2], first, last - first, passed)

    lane_k = iota((width, 128), 1)
    sub = iota((pad, 128), 0)
    sub_f = sub.astype(F32)
    empty = jnp.zeros((width, 128), F32)

    def slots_of(group):
        first, last = groups[group]
        return [(place, slot) for place in range(first, last) for slot in range(slots)]

    def product(tile, row):
        return jnp.sum(tile * row, axis=1, keepdims=True)

    def turn_over(vector):
        filled = jnp.concatenate([vector, jnp.zeros((width - pad, 128), F32)], axis=0)
        return filled.T

    def spread(turned):
        for index in range(rb):
            held[index] = jnp.broadcast_to(turned[:, index : index + 1], (width, 128))

    def push_group(turn, group):
        for place, slot in slots_of(group):
            line = place * slots + slot
            value = far_t[line] * held[table[4, line]]
            send_b[turn, line, :, :] = jnp.sum(value, axis=0, keepdims=True)
        send(1 + 2 * turn, group, send_b.at[turn], recv_b.at[turn], slots, True)

    ones = jnp.ones((2 * width, 128), jnp.bfloat16)

    def product_too(tile, row):
        value = tile * row
        high = value.astype(jnp.bfloat16)
        rest = (value - high.astype(F32)).astype(jnp.bfloat16)
        return jnp.dot(
            jnp.concatenate([high, rest], axis=1), ones, preferred_element_type=F32
        )

    def own_rows(image):
        for index in range(rb):
            value = jnp.sum(diag_t[index] * held[index], axis=0, keepdims=True)
            image = image + jnp.where(sub == index, value, 0.0)
        return image

    def fetch_all(image, ready, source, between):
        acc = empty
        for group in near_first:
            ready(group)
            for index, (place, slot) in enumerate(slots_of(group)):
                line = place * slots + slot
                by = product_too if group > 0 and index % 3 == 1 else product
                value = by(coup[table[0, line]], source(place, slot))
                acc = acc + jnp.where(lane_k == table[1, line], value, 0.0)
            image = between(group, image)
        return image + acc.T[0:pad, :]

    def land_group(turn, group, image):
        for place, slot in slots_of(group):
            here = goal_ref[slot, place : place + 1, :] == sub_f
            line = recv_b[turn, place * slots + slot, :, :]
            image = image + jnp.where(here, line, 0.0)
        return image

    def decode(first, last):
        shape = (last - first, 128)
        found = codes[first:last, :]
        lane = iota(shape, 1)
        for slot in range(slots):
            mine = jnp.where(lane == me * slots + slot, found, 0.0)
            value = jnp.sum(mine, axis=1, keepdims=True)
            goal = jnp.floor(value * (1.0 / BASE))
            goal_ref[slot, first:last, :] = jnp.broadcast_to(goal - 1.0, shape)
            ask_ref[slot, first:last, :] = jnp.broadcast_to(value - goal * BASE - 1.0, shape)

    def gather_group(turn, group, vector):
        for place, slot in slots_of(group):
            here = ask_ref[slot, place : place + 1, :] == sub_f
            line = jnp.sum(jnp.where(here, vector, 0.0), axis=0, keepdims=True)
            send_a[turn - 1, place * lines + slot, :, :] = line

    def send_asked(turn, group, own_part):
        for place in range(*groups[group]):
            send_a[turn - 1, place * lines + slots, :, :] = own_part
        send(2 * turn, group, send_a.at[turn - 1], recv_a.at[turn - 1], lines, True)

    for item in loads:
        item.wait()
    table_copy.wait()
    mass = jnp.concatenate([mass_ref[...], jnp.zeros((pad - rb, 128), F32)], axis=0)

    urgent = list(range(count))
    cut = min(-(-groups[min(1, count - 1)][1] // 8) * 8, n)
    early = [group for group in reversed(range(count)) if groups[group][0] >= cut]
    near_first = list(reversed(range(count)))
    spread(turn_over(vector))
    for group in range(count):
        for place, slot in slots_of(group):
            line = place * slots + slot
            far_t[line] = coup[table[3, line]].T
        push_group(0, group)
    for index in range(rb):
        diag_t[index] = diag[index].T
    image = own_rows(mass * vector)
    landed = {2: near_first[:2], 1: near_first[2:-2]} if count > 3 else {1: near_first[:-2]}

    def ready_first(group):
        if group == 1:
            take_first(1)
            take_first(0)
        elif group > 1 or count == 1:
            take_first(group)

    def take_first(group):
        await_group(0, group, recv0, head)
        if group not in plain:
            pl.when(core == 1)(pass_on(group).start)
        for place in range(*groups[group]):
            spot = place
            if place < n - 2 and group not in plain:
                spot = place + (1 - core) * (1 - 2 * (place % 2))
            codes[place : place + 1, :] = recv0[spot * head + rb]
            for row in range(rb):
                blocks[place * rb + row, :, :] = recv0[spot * head + row]

    def block_row(place, slot):
        return blocks[place * rb + table[2, place * slots + slot]]

    def between_first(group, image):
        if group == 0:
            if cut < n:
                decode(cut, n)
            for other in early:
                await_group(1, other, recv_b.at[0], slots)
                image = land_group(0, other, image)
        return image

    image = fetch_all(image, ready_first, block_row, between_first)
    decode(0, cut)
    places = iota((n, 1), 0)
    whose = sum(jnp.where(places == at, mask, 0) for at, mask in enumerate(masks)) ^ me
    squares = total(jnp.where(iota((n, 128), 1) == whose * slots, codes[...], 0.0))
    beta = jnp.sqrt(squares)
    for group in near_first:
        if group in early:
            continue
        await_group(1, group, recv_b.at[0], slots)
        image = land_group(0, group, image)
    basis = [vector / beta]
    images = [image / beta]
    heads = []
    gram = {}

    for turn in range(1, ITERS):
        vector = images[-1]
        own_part = as_row(
            [total(vector * item) for item in basis]
            + [total(vector * item) for item in images]
        )
        turned = turn_over(vector)
        for group in urgent:
            gather_group(turn, group, vector)
            send_asked(turn, group, own_part)
        spread(turned)
        for group in urgent[:2]:
            push_group(turn, group)
        for group in range(len(urgent), count):
            gather_group(turn, group, vector)
            send_asked(turn, group, own_part)
        for group in range(len(urgent[:2]), count):
            push_group(turn, group)
        image = own_rows(mass * vector)
        parts_of = [own_part]

        def ready(group):
            await_group(2 * turn, group, recv_a.at[turn - 1], lines)
            for place in range(*groups[group]):
                parts_of.append(recv_a[turn - 1, place * lines + slots, :, :])

        def asked_row(place, slot):
            return recv_a[turn - 1, place * lines + slot, :, :]

        def between(group, image):
            for other in landed.get(group, ()):
                await_group(1 + 2 * turn, other, recv_b.at[turn], slots)
                image = land_group(turn, other, image)
            return image

        image = fetch_all(image, ready, asked_row, between)
        sums = sum(parts_of[1:], parts_of[0])
        dots = [pick(sums, index) for index in range(turn)]
        for index in range(turn):
            gram[index, turn - 1] = pick(sums, turn + index)
        heads.append(dots[0])
        square = gram[turn - 1, turn - 1]
        left = square
        for value in dots:
            left = left - value * value
        scale = lax.rsqrt(jnp.maximum(left, square * 1e-6))
        for index in range(turn):
            vector = vector - dots[index] * basis[index]
        basis.append(vector * scale)
        for group in near_first[-2:]:
            await_group(1 + 2 * turn, group, recv_b.at[turn], slots)
            image = land_group(turn, group, image)
        for index in range(turn):
            image = image - dots[index] * images[index]
        images.append(image * scale)

    vector = images[-1]
    own_part = as_row(
        [total(vector * basis[0])] + [total(vector * item) for item in images]
    )
    send_f[0] = own_part
    last_phase = 2 * ITERS
    for group in range(count):
        send(last_phase, group, send_f, recv_f, 1, False)
    extra = n - 2 - groups[plain[0]][0]
    view = recv0.at[pl.ds(0, (n // 2 + extra // 2) * head)]
    pltpu.make_async_copy(view, view, sent.at[0]).wait()
    whole = recv0.at[pl.ds(0, (n - 2 - extra) * head)]
    pl.when(core == 1)(pltpu.make_async_copy(whole, whole, passed).wait)
    for turn in range(ITERS):
        await_sent(1 + 2 * turn, recv_b.at[turn], slots)
    for turn in range(1, ITERS):
        await_sent(2 * turn, recv_a.at[turn - 1], lines)
    factor = {}
    forward = []

    def eliminate(i):
        for j in range(i + 1):
            value = gram[j, i]
            for k in range(j):
                value = value - factor[i, k] * factor[j, k]
            factor[i, j] = jnp.sqrt(value) if i == j else value / factor[j, j]
        value = beta * heads[i]
        for k in range(i):
            value = value - factor[i, k] * forward[k]
        forward.append(value / factor[i, i])

    for i in range(ITERS - 1):
        eliminate(i)
    sums = own_part
    for group in near_first:
        await_group(last_phase, group, recv_f, 1)
        for place in range(*groups[group]):
            sums = sums + recv_f[place, :, :]
    heads.append(pick(sums, 0))
    for index in range(ITERS):
        gram[index, ITERS - 1] = pick(sums, 1 + index)

    eliminate(ITERS - 1)
    mixing = [None] * ITERS
    for i in reversed(range(ITERS)):
        value = forward[i]
        for k in range(i + 1, ITERS):
            value = value - factor[k, i] * mixing[k]
        mixing[i] = value / factor[i, i]
    update = mixing[0] * basis[0]
    for i in range(1, ITERS):
        update = update + mixing[i] * basis[i]
    out_ref[...] = update[0:rb, :]

    await_sent(last_phase, recv_f, 1)


def on_device(defect, mass, block_diag, coupling, tile_rows, tile_cols):
    rb, width = defect.shape
    tiles = tile_rows.shape[0]
    n = lax.axis_size("blk")
    slots = (tiles // 2 + n - 2) // (n - 1)
    lines = slots + 1
    pad = -(-rb // 8) * 8
    lanes = -(-n * slots // 128) * 128
    hbm = pl.BlockSpec(memory_space=pltpu.HBM)
    phases = 2 * ITERS + 1
    return pl.pallas_call(
        functools.partial(kernel, n, slots),
        out_shape=pltpu.VMEM((rb, width), F32),
        in_specs=[hbm] * 6,
        out_specs=pl.BlockSpec(memory_space=pltpu.VMEM),
        scratch_shapes=[
            pltpu.VMEM((tiles, width, width), F32),
            pltpu.VMEM((rb, width, width), F32),
            pltpu.VMEM((rb, width), F32),
            pltpu.VMEM((rb, width), F32),
            pltpu.VMEM((1, tiles), I32),
            pltpu.VMEM((1, tiles), I32),
            pltpu.VMEM((8, lanes), I32),
            pltpu.SMEM((8, lanes), I32),
            pltpu.VMEM((pad, width), F32),
            pltpu.VMEM((rb, width, width), F32),
            pltpu.VMEM(((n - 1) * slots, width, width), F32),
            pltpu.VMEM((rb, width, width), F32),
            pltpu.VMEM((n, width), F32),
            pltpu.VMEM((slots, n, width), F32),
            pltpu.VMEM((slots, n, width), F32),
            pltpu.VMEM((rb + 1, 1, width), F32),
            pltpu.VMEM((n * (rb + 1), 1, width), F32),
            pltpu.VMEM((n * rb, 1, width), F32),
            pltpu.VMEM((ITERS - 1, n * lines, 1, width), F32),
            pltpu.VMEM((ITERS - 1, n * lines, 1, width), F32),
            pltpu.VMEM((ITERS, n * slots, 1, width), F32),
            pltpu.VMEM((ITERS, n * slots, 1, width), F32),
            pltpu.VMEM((1, 1, width), F32),
            pltpu.VMEM((n, 1, width), F32),
            pltpu.SemaphoreType.DMA((9,)),
            pltpu.SemaphoreType.DMA,
            pltpu.SemaphoreType.DMA((phases,)),
            pltpu.SemaphoreType.DMA,
            pltpu.SemaphoreType.DMA((phases, len(layout(n)[1]))),
        ],
        compiler_params=pltpu.CompilerParams(
            collective_id=0, has_side_effects=True, vmem_limit_bytes=VMEM_LIMIT
        ),
    )(
        defect,
        mass,
        block_diag,
        coupling,
        tile_rows.reshape(1, tiles),
        tile_cols.reshape(1, tiles),
    )


def solution(mesh):
    in_specs = (
        P("blk", None),
        P("blk", None),
        P("blk", None, None),
        P("blk", None, None),
        P("blk"),
        P("blk"),
    )
    return jax.shard_map(
        on_device, mesh=mesh, in_specs=in_specs, out_specs=P("blk", None), check_vma=False
    )
```

```python
import functools

import jax
import jax.numpy as jnp
from jax import lax
from jax.experimental import pallas as pl
from jax.experimental.pallas import tpu as pltpu
from jax.sharding import PartitionSpec as P

ITERS = 3
F32 = jnp.float32
I32 = jnp.int32
MESH = pl.DeviceIdType.MESH
BASE = 64
VMEM_LIMIT = 57 * 1024 * 1024


def iota(shape, axis):
    return lax.broadcasted_iota(I32, shape, axis)


def iota_f(shape, axis):
    return iota(shape, axis).astype(F32)


def total(value):
    return jnp.sum(jnp.sum(value, axis=0, keepdims=True), axis=1, keepdims=True)


def as_row(items):
    lane = iota((1, 128), 1)
    row = jnp.zeros((1, 128), F32)
    for index, item in enumerate(items):
        row = jnp.where(lane == index, item, row)
    return row


def pick(row, index):
    lane = iota((1, 128), 1)
    return jnp.sum(jnp.where(lane == index, row, 0.0), axis=1, keepdims=True)


def layout(n):
    def far(chip):
        return min((chip & 1) + (chip >> 1 & 1) + (chip >> 2), 5)

    chips = sorted(range(n // 2), key=lambda chip: (-far(chip), -chip))
    masks = [2 * chip + bit for chip in chips for bit in (1, 0)]
    levels = [max(far(mask // 2), 1) for mask in masks[: n - 1]]
    starts = [at for at in range(n - 1) if at == 0 or levels[at] != levels[at - 1]]
    return masks, list(zip(starts, starts[1:] + [n - 1]))


def kernel(
    n,
    slots,
    defect_hbm,
    mass_hbm,
    diag_hbm,
    coup_hbm,
    rows_hbm,
    cols_hbm,
    out_ref,
    coup,
    diag,
    defect_ref,
    mass_ref,
    rows_ref,
    cols_ref,
    table_v,
    table,
    wbuf,
    held,
    far_t,
    diag_t,
    codes,
    ask_ref,
    goal_ref,
    send0,
    recv0,
    blocks,
    send_a,
    recv_a,
    send_b,
    recv_b,
    send_f,
    recv_f,
    load_sems,
    table_sem,
    sent,
    passed,
    got,
):
    me = lax.axis_index("blk")
    rb, width = defect_ref.shape
    tiles = rows_ref.shape[1]
    pad = wbuf.shape[0]
    lanes = table.shape[1]
    parts = 4
    chunk = tiles // parts
    masks, groups = layout(n)
    count = len(groups)
    head = rb + 1
    lines = slots + 1

    peers = {0: me}
    for mask in range(1, n):
        low_bit = mask & -mask
        sign = 1 - 2 * ((me // low_bit) % 2)
        peers[mask] = peers[mask - low_bit] + sign * low_bit
    peer = [peers[mask] for mask in masks]

    small = [
        pltpu.make_async_copy(rows_hbm, rows_ref, load_sems.at[parts + 1]),
        pltpu.make_async_copy(cols_hbm, cols_ref, load_sems.at[parts + 2]),
        pltpu.make_async_copy(defect_hbm, defect_ref, load_sems.at[parts + 3]),
        pltpu.make_async_copy(mass_hbm, mass_ref, load_sems.at[parts + 4]),
    ]
    for item in small:
        item.start()

    barrier = pltpu.get_barrier_semaphore()
    for place in range(n - 1):
        pl.semaphore_signal(barrier, inc=1, device_id=(peer[place],), device_id_type=MESH)

    loads = []
    for part in range(parts):
        span = pl.ds(part * chunk, chunk)
        loads.append(
            pltpu.make_async_copy(coup_hbm.at[span], coup.at[span], load_sems.at[part])
        )
    loads.append(pltpu.make_async_copy(diag_hbm, diag, load_sems.at[parts]))
    for item in loads:
        item.start()
    for item in small:
        item.wait()

    rows = rows_ref[...]
    cols = cols_ref[...]
    low = me * rb
    pushes = (rows < low) | (rows >= low + rb)
    push_l = jnp.where(pushes, 1, 0)
    rem_l = jnp.where(pushes, rows, cols)
    loc_l = jnp.where(pushes, cols, rows) - low
    own_l = (rem_l * (-(-65536 // rb))) >> 16
    far_l = rem_l - own_l * rb
    square = (tiles, tiles)
    eye = iota(square, 0) == iota(square, 1)
    earlier = iota(square, 0) < iota(square, 1)

    def to_s(value, zero):
        return jnp.sum(jnp.where(eye, value, zero), axis=1, keepdims=True)

    key_l = own_l + push_l * n
    key_s = to_s(key_l, 0)
    slot_l = jnp.sum(jnp.where((key_s == key_l) & earlier, 1, 0), axis=0, keepdims=True)
    apart = own_l ^ me
    place_l = sum(jnp.where(apart == mask, at, 0) for at, mask in enumerate(masks))
    line_l = place_l * slots + slot_l
    tile_l = iota((1, tiles), 1)
    line_s = to_s(line_l + push_l * lanes, 0)
    pack_s = to_s(((tile_l * BASE + loc_l) * BASE + far_l) + 1, 0)
    name_s = to_s(own_l * slots + slot_l, 0)
    code_s = to_s(jnp.where(pushes, (far_l + 1) * BASE, far_l + 1).astype(F32), 0.0)
    wide = (tiles, lanes)
    lane_w = iota(wide, 1)
    kinds = []
    for kind in range(2):
        here = line_s == lane_w + kind * lanes
        packed = jnp.sum(jnp.where(here, pack_s, 0), axis=0, keepdims=True)
        there = packed > 0
        packed = jnp.where(there, packed - 1, 0)
        local = jnp.clip((packed >> 6) & (BASE - 1), 0, rb - 1)
        kinds.append(jnp.clip(packed >> 12, 0, tiles - 1))
        kinds.append(jnp.where(there, local, BASE) if kind == 0 else local)
        if kind == 0:
            kinds.append(jnp.clip(packed & (BASE - 1), 0, rb - 1))
    for index, value in enumerate(kinds):
        table_v[index : index + 1, :] = value
    table_copy = pltpu.make_async_copy(table_v, table, table_sem)
    table_copy.start()
    code = jnp.sum(jnp.where(name_s == lane_w, code_s, 0.0), axis=0, keepdims=True)
    code = code[:, 0:128]

    wbuf[...] = jnp.zeros(wbuf.shape, F32)
    wbuf[0:rb, :] = -defect_ref[...]
    vector = wbuf[...]
    lane_1 = iota((1, 128), 1)
    code = jnp.where(lane_1 == me * slots, total(vector * vector), code)
    send0[0:rb, 0, :] = -defect_ref[...]
    send0[rb, :, :] = code
    codes[n - 1 : n, :] = code

    pl.semaphore_wait(barrier, n - 1)

    def send(phase, group, source, target, size, spread):
        for place in range(*groups[group]):
            span = pl.ds(place * size, size)
            pltpu.make_async_remote_copy(
                src_ref=source.at[span] if spread else source,
                dst_ref=target.at[span],
                send_sem=sent.at[phase],
                recv_sem=got.at[phase, group],
                device_id=(peer[place],),
                device_id_type=MESH,
            ).start()

    def await_group(phase, group, target, size):
        first, last = groups[group]
        view = target.at[pl.ds(first * size, (last - first) * size)]
        pltpu.make_async_copy(view, view, got.at[phase, group]).wait()

    def await_sent(phase, target, size):
        view = target.at[pl.ds(0, (n - 1) * size)]
        pltpu.make_async_copy(view, view, sent.at[phase]).wait()

    core = me % 2

    def first_copy(source, group, device, spot, size, sem):
        return pltpu.make_async_remote_copy(
            src_ref=source,
            dst_ref=recv0.at[pl.ds(spot * head, size * head)],
            send_sem=sem,
            recv_sem=got.at[0, group],
            device_id=(device,),
            device_id_type=MESH,
        )

    plain = [group for group in range(count) if group >= count - 2]
    for group in range(count):
        if group in plain:
            for place in range(*groups[group]):
                first_copy(send0, group, peer[place], place, 1, sent.at[0]).start()
            continue
        for place in range(groups[group][0], groups[group][1], 2):
            if place < n - 2:
                device, spot = peer[place + 1] + 1 - core, place + core
            else:
                device, spot = peer[place], place
            first_copy(send0, group, device, spot, 1, sent.at[0]).start()

    def pass_on(group):
        first, last = groups[group]
        last = min(last, n - 2)
        part = recv0.at[pl.ds(first * head, (last - first) * head)]
        return first_copy(part, group, peer[n - 2], first, last - first, passed)

    lane_k = iota((width, 128), 1)
    sub = iota((pad, 128), 0)
    sub_f = sub.astype(F32)
    empty = jnp.zeros((width, 128), F32)

    def slots_of(group):
        first, last = groups[group]
        return [(place, slot) for place in range(first, last) for slot in range(slots)]

    def product(tile, row):
        return jnp.sum(tile * row, axis=1, keepdims=True)

    def turn_over(vector):
        filled = jnp.concatenate([vector, jnp.zeros((width - pad, 128), F32)], axis=0)
        return filled.T

    def spread(turned):
        for index in range(rb):
            held[index] = jnp.broadcast_to(turned[:, index : index + 1], (width, 128))

    def push_group(turn, group):
        for place, slot in slots_of(group):
            line = place * slots + slot
            value = far_t[line] * held[table[4, line]]
            send_b[turn, line, :, :] = jnp.sum(value, axis=0, keepdims=True)
        send(1 + 2 * turn, group, send_b.at[turn], recv_b.at[turn], slots, True)

    ones = jnp.ones((2 * width, 128), jnp.bfloat16)

    def product_too(tile, row):
        value = tile * row
        high = value.astype(jnp.bfloat16)
        rest = (value - high.astype(F32)).astype(jnp.bfloat16)
        return jnp.dot(
            jnp.concatenate([high, rest], axis=1), ones, preferred_element_type=F32
        )

    def own_rows(image):
        for index in range(rb):
            value = jnp.sum(diag_t[index] * held[index], axis=0, keepdims=True)
            image = image + jnp.where(sub == index, value, 0.0)
        return image

    def fetch_all(image, ready, source, between):
        acc = empty
        for group in near_first:
            ready(group)
            for index, (place, slot) in enumerate(slots_of(group)):
                line = place * slots + slot
                by = product_too if group > 0 and index % 3 == 1 else product
                value = by(coup[table[0, line]], source(place, slot))
                acc = acc + jnp.where(lane_k == table[1, line], value, 0.0)
            image = between(group, image)
        return image + acc.T[0:pad, :]

    def land_group(turn, group, image):
        for place, slot in slots_of(group):
            here = goal_ref[slot, place : place + 1, :] == sub_f
            line = recv_b[turn, place * slots + slot, :, :]
            image = image + jnp.where(here, line, 0.0)
        return image

    def decode(first, last):
        shape = (last - first, 128)
        found = codes[first:last, :]
        lane = iota(shape, 1)
        for slot in range(slots):
            mine = jnp.where(lane == me * slots + slot, found, 0.0)
            value = jnp.sum(mine, axis=1, keepdims=True)
            goal = jnp.floor(value * (1.0 / BASE))
            goal_ref[slot, first:last, :] = jnp.broadcast_to(goal - 1.0, shape)
            ask_ref[slot, first:last, :] = jnp.broadcast_to(value - goal * BASE - 1.0, shape)

    def gather_group(turn, group, vector):
        for place, slot in slots_of(group):
            here = ask_ref[slot, place : place + 1, :] == sub_f
            line = jnp.sum(jnp.where(here, vector, 0.0), axis=0, keepdims=True)
            send_a[turn - 1, place * lines + slot, :, :] = line

    def send_asked(turn, group, own_part):
        for place in range(*groups[group]):
            send_a[turn - 1, place * lines + slots, :, :] = own_part
        send(2 * turn, group, send_a.at[turn - 1], recv_a.at[turn - 1], lines, True)

    for item in loads:
        item.wait()
    table_copy.wait()
    mass = jnp.concatenate([mass_ref[...], jnp.zeros((pad - rb, 128), F32)], axis=0)

    urgent = list(range(count))
    cut = min(-(-groups[min(1, count - 1)][1] // 8) * 8, n)
    early = [group for group in reversed(range(count)) if groups[group][0] >= cut]
    near_first = list(reversed(range(count)))
    spread(turn_over(vector))
    for group in range(count):
        for place, slot in slots_of(group):
            line = place * slots + slot
            far_t[line] = coup[table[3, line]].T
        push_group(0, group)
    for index in range(rb):
        diag_t[index] = diag[index].T
    image = own_rows(mass * vector)
    landed = {2: near_first[:2], 1: near_first[2:-2]} if count > 3 else {1: near_first[:-2]}

    def ready_first(group):
        if group == 1:
            take_first(1)
            take_first(0)
        elif group > 1 or count == 1:
            take_first(group)

    def take_first(group):
        await_group(0, group, recv0, head)
        if group not in plain:
            pl.when(core == 1)(pass_on(group).start)
        for place in range(*groups[group]):
            spot = place
            if place < n - 2 and group not in plain:
                spot = place + (1 - core) * (1 - 2 * (place % 2))
            codes[place : place + 1, :] = recv0[spot * head + rb]
            for row in range(rb):
                blocks[place * rb + row, :, :] = recv0[spot * head + row]

    def block_row(place, slot):
        return blocks[place * rb + table[2, place * slots + slot]]

    def between_first(group, image):
        if group == 0:
            if cut < n:
                decode(cut, n)
            for other in early:
                await_group(1, other, recv_b.at[0], slots)
                image = land_group(0, other, image)
        return image

    image = fetch_all(image, ready_first, block_row, between_first)
    decode(0, cut)
    places = iota((n, 1), 0)
    whose = sum(jnp.where(places == at, mask, 0) for at, mask in enumerate(masks)) ^ me
    squares = total(jnp.where(iota((n, 128), 1) == whose * slots, codes[...], 0.0))
    beta = jnp.sqrt(squares)
    for group in near_first:
        if group in early:
            continue
        await_group(1, group, recv_b.at[0], slots)
        image = land_group(0, group, image)
    basis = [vector / beta]
    images = [image / beta]
    heads = []
    gram = {}

    for turn in range(1, ITERS):
        vector = images[-1]
        own_part = as_row(
            [total(vector * item) for item in basis]
            + [total(vector * item) for item in images]
        )
        turned = turn_over(vector)
        for group in urgent:
            gather_group(turn, group, vector)
            send_asked(turn, group, own_part)
        spread(turned)
        for group in urgent[:2]:
            push_group(turn, group)
        for group in range(len(urgent), count):
            gather_group(turn, group, vector)
            send_asked(turn, group, own_part)
        for group in range(len(urgent[:2]), count):
            push_group(turn, group)
        image = own_rows(mass * vector)
        parts_of = [own_part]

        def ready(group):
            await_group(2 * turn, group, recv_a.at[turn - 1], lines)
            for place in range(*groups[group]):
                parts_of.append(recv_a[turn - 1, place * lines + slots, :, :])

        def asked_row(place, slot):
            return recv_a[turn - 1, place * lines + slot, :, :]

        def between(group, image):
            for other in landed.get(group, ()):
                await_group(1 + 2 * turn, other, recv_b.at[turn], slots)
                image = land_group(turn, other, image)
            return image

        image = fetch_all(image, ready, asked_row, between)
        sums = sum(parts_of[1:], parts_of[0])
        dots = [pick(sums, index) for index in range(turn)]
        for index in range(turn):
            gram[index, turn - 1] = pick(sums, turn + index)
        heads.append(dots[0])
        square = gram[turn - 1, turn - 1]
        left = square
        for value in dots:
            left = left - value * value
        scale = lax.rsqrt(jnp.maximum(left, square * 1e-6))
        for index in range(turn):
            vector = vector - dots[index] * basis[index]
        basis.append(vector * scale)
        for group in near_first[-2:]:
            await_group(1 + 2 * turn, group, recv_b.at[turn], slots)
            image = land_group(turn, group, image)
        for index in range(turn):
            image = image - dots[index] * images[index]
        images.append(image * scale)

    vector = images[-1]
    own_part = as_row(
        [total(vector * basis[0])] + [total(vector * item) for item in images]
    )
    send_f[0] = own_part
    last_phase = 2 * ITERS
    for group in range(count):
        send(last_phase, group, send_f, recv_f, 1, False)
    extra = n - 2 - groups[plain[0]][0]
    view = recv0.at[pl.ds(0, (n // 2 + extra // 2) * head)]
    pltpu.make_async_copy(view, view, sent.at[0]).wait()
    whole = recv0.at[pl.ds(0, (n - 2 - extra) * head)]
    pl.when(core == 1)(pltpu.make_async_copy(whole, whole, passed).wait)
    for turn in range(ITERS):
        await_sent(1 + 2 * turn, recv_b.at[turn], slots)
    for turn in range(1, ITERS):
        await_sent(2 * turn, recv_a.at[turn - 1], lines)
    factor = {}
    forward = []

    def eliminate(i):
        for j in range(i + 1):
            value = gram[j, i]
            for k in range(j):
                value = value - factor[i, k] * factor[j, k]
            factor[i, j] = jnp.sqrt(value) if i == j else value / factor[j, j]
        value = beta * heads[i]
        for k in range(i):
            value = value - factor[i, k] * forward[k]
        forward.append(value / factor[i, i])

    for i in range(ITERS - 1):
        eliminate(i)
    sums = own_part
    for group in near_first:
        await_group(last_phase, group, recv_f, 1)
        for place in range(*groups[group]):
            sums = sums + recv_f[place, :, :]
    heads.append(pick(sums, 0))
    for index in range(ITERS):
        gram[index, ITERS - 1] = pick(sums, 1 + index)

    eliminate(ITERS - 1)
    mixing = [None] * ITERS
    for i in reversed(range(ITERS)):
        value = forward[i]
        for k in range(i + 1, ITERS):
            value = value - factor[k, i] * mixing[k]
        mixing[i] = value / factor[i, i]
    update = mixing[0] * basis[0]
    for i in range(1, ITERS):
        update = update + mixing[i] * basis[i]
    out_ref[...] = update[0:rb, :]

    await_sent(last_phase, recv_f, 1)


def on_device(defect, mass, block_diag, coupling, tile_rows, tile_cols):
    rb, width = defect.shape
    tiles = tile_rows.shape[0]
    n = lax.axis_size("blk")
    slots = (tiles // 2 + n - 2) // (n - 1)
    lines = slots + 1
    pad = -(-rb // 8) * 8
    lanes = -(-n * slots // 128) * 128
    hbm = pl.BlockSpec(memory_space=pltpu.HBM)
    phases = 2 * ITERS + 1
    return pl.pallas_call(
        functools.partial(kernel, n, slots),
        out_shape=pltpu.VMEM((rb, width), F32),
        in_specs=[hbm] * 6,
        out_specs=pl.BlockSpec(memory_space=pltpu.VMEM),
        scratch_shapes=[
            pltpu.VMEM((tiles, width, width), F32),
            pltpu.VMEM((rb, width, width), F32),
            pltpu.VMEM((rb, width), F32),
            pltpu.VMEM((rb, width), F32),
            pltpu.VMEM((1, tiles), I32),
            pltpu.VMEM((1, tiles), I32),
            pltpu.VMEM((8, lanes), I32),
            pltpu.SMEM((8, lanes), I32),
            pltpu.VMEM((pad, width), F32),
            pltpu.VMEM((rb, width, width), F32),
            pltpu.VMEM(((n - 1) * slots, width, width), F32),
            pltpu.VMEM((rb, width, width), F32),
            pltpu.VMEM((n, width), F32),
            pltpu.VMEM((slots, n, width), F32),
            pltpu.VMEM((slots, n, width), F32),
            pltpu.VMEM((rb + 1, 1, width), F32),
            pltpu.VMEM((n * (rb + 1), 1, width), F32),
            pltpu.VMEM((n * rb, 1, width), F32),
            pltpu.VMEM((ITERS - 1, n * lines, 1, width), F32),
            pltpu.VMEM((ITERS - 1, n * lines, 1, width), F32),
            pltpu.VMEM((ITERS, n * slots, 1, width), F32),
            pltpu.VMEM((ITERS, n * slots, 1, width), F32),
            pltpu.VMEM((1, 1, width), F32),
            pltpu.VMEM((n, 1, width), F32),
            pltpu.SemaphoreType.DMA((9,)),
            pltpu.SemaphoreType.DMA,
            pltpu.SemaphoreType.DMA((phases,)),
            pltpu.SemaphoreType.DMA,
            pltpu.SemaphoreType.DMA((phases, len(layout(n)[1]))),
        ],
        compiler_params=pltpu.CompilerParams(
            collective_id=0, has_side_effects=True, vmem_limit_bytes=VMEM_LIMIT
        ),
    )(
        defect,
        mass,
        block_diag,
        coupling,
        tile_rows.reshape(1, tiles),
        tile_cols.reshape(1, tiles),
    )


def solution(mesh):
    in_specs = (
        P("blk", None),
        P("blk", None),
        P("blk", None, None),
        P("blk", None, None),
        P("blk"),
        P("blk"),
    )
    return jax.shard_map(
        on_device, mesh=mesh, in_specs=in_specs, out_specs=P("blk", None), check_vma=False
    )
```
